256 devices in a mesh: dom: 32 (over y, z), sub: 8 (over x, core).
Axes of the slice: x: 4, y: 4, z: 8, core: 2. Of those that a mesh axis runs over, the one named last changes fastest.
Arguments:
- positions: float32 [16384, 3, 256], P(('dom', 'sub')), may hold values from -6 to 6
- time_bins: int32 [16384, 256], P(('dom', 'sub')), may hold values from 0 to 5
- home_groups: int32 [16384], P(('dom', 'sub')), may hold values from 0 to 63
- targets: int32 [16384, 4], P(('dom', 'sub')), may hold values from -1 to 31, as said below
- target_groups: int32 [16384, 4], P(('dom', 'sub')), may hold values from 0 to 63
- node_pos: float32 [3, 1048576], P(None, ('dom', 'sub')), may hold values from -6 to 6
- node_mass: float32 [1048576], P(('dom', 'sub')), may hold values from 0.2 to 2
- node_lists: int32 [2048, 256], P('dom'), may hold values from 0 to 32767
- list_counts: int32 [2048], P('dom'), may hold values from 64 to 256, as said below
Outputs:
- forces: float32 [16384, 3, 256], P(('dom', 'sub'))
The draws below stay inside these ranges and needn't reach their ends.
Inputs may be any that keep to these rules, and one draw needn't show every extreme that they name: `targets`: row b names the remote domains that block b visits, each at most once and never its own domain b // 512; -1 marks an unused entry, in any column. The rows of one device name one domain at most 8 times, and some device names some domain exactly 8 times in every draw. The rows of one domain's 8 devices together name one domain at most 16 times, and this is reached in every draw. `list_counts`: each domain has at least one list with all 256 entries valid.
All inputs are finite; a program needn't handle non-finite values.
Results may differ from the reference program's by a relative error of at most 0.0003.
Values sent between devices are 32-bit elements; how exact they have to be, the bound alone decides.
A program may use at most 128 MiB of HBM per device.

```python
import math
import jax
import jax.numpy as jnp
from jax import lax

BLOCK = 256
BLK_DEV = 64
TOP = 4
LIST = 256
GROUPS = 64
NODE_DEV = 4096
BINS = 6
CUR_BIN = 2
BLOCKS = 16384
NODES = 1048576
CAP = 8
CAP_ROW = 16
N_DOM = 32
N_SUB = 8


def draw_list_counts(key, part):
    count_key = jax.random.fold_in(key, 11)
    full_key = jax.random.fold_in(key, 12)
    counts = jax.random.randint(count_key, (N_DOM, GROUPS), LIST // 4, LIST + 1)
    full_list = jax.random.randint(full_key, (N_DOM,), 0, GROUPS)
    counts = jnp.where(jnp.arange(GROUPS)[None, :] == full_list[:, None], LIST, counts)
    return counts.reshape(N_DOM * GROUPS).astype(jnp.int32)


def draw_targets(key, part):
    hot_key = jax.random.fold_in(key, 21)
    order_key = jax.random.fold_in(key, 22)
    level_key = jax.random.fold_in(key, 23)
    wish_key = jax.random.fold_in(key, 24)
    block_key = jax.random.fold_in(key, 25)
    column_key = jax.random.fold_in(key, 26)
    hot_domain = jax.random.randint(hot_key, (), 0, N_DOM)
    domain_ids = jnp.arange(N_DOM, dtype=jnp.int32)
    orders = jax.vmap(lambda one_key: jax.random.permutation(one_key, N_SUB))(jax.random.split(order_key, N_DOM))
    levels = jax.random.randint(level_key, (N_DOM, N_SUB, 1), 0, 4)
    wishes = jnp.minimum(CAP, jax.random.randint(wish_key, (N_DOM, N_SUB, N_DOM), 0, CAP + 1) * levels // 2)
    wishes = jnp.where(domain_ids[None, None, :] == hot_domain, CAP, wishes)
    wishes = jnp.where(domain_ids[:, None, None] == domain_ids[None, None, :], 0, wishes).astype(jnp.int32)
    rotation = (hot_domain + domain_ids) % N_DOM
    unrotate = (domain_ids - hot_domain) % N_DOM
    budget = BLK_DEV * TOP

    def row_counts(row_wishes, row_order):

        def advance(already, position):
            wanted = jnp.minimum(row_wishes[row_order[position]], CAP_ROW - already)
            turned = wanted[rotation]
            before = jnp.cumsum(turned) - turned
            granted = jnp.maximum(jnp.minimum(turned, budget - before), 0)[unrotate]
            return (already + granted, granted)
        _, granted = lax.scan(advance, jnp.zeros((N_DOM,), jnp.int32), jnp.arange(N_SUB))
        return jnp.zeros((N_SUB, N_DOM), jnp.int32).at[row_order].set(granted)
    counts = jax.vmap(row_counts)(wishes, orders).reshape(N_DOM * N_SUB, N_DOM)
    tickets = jnp.arange(budget, dtype=jnp.int32)

    def device_table(device_counts, shuffle_key, order_keys):
        boundaries = jnp.cumsum(device_counts)
        ticket_domain = jnp.sum((boundaries[None, :] <= tickets[:, None]).astype(jnp.int32), axis=1)
        ticket_domain = jnp.where(tickets < boundaries[-1], ticket_domain, -1)
        assigned = ticket_domain.reshape(TOP, BLK_DEV).T
        assigned = assigned[jax.random.permutation(shuffle_key, BLK_DEV)]
        column_orders = jax.vmap(lambda one_key: jax.random.permutation(one_key, TOP))(jax.random.split(order_keys, BLK_DEV))
        return jnp.take_along_axis(assigned, column_orders, axis=1)
    device_total = N_DOM * N_SUB
    tables = jax.vmap(device_table)(counts, jax.random.split(block_key, device_total), jax.random.split(column_key, device_total))
    return tables.reshape(device_total * BLK_DEV, TOP).astype(jnp.int32)


def set_ends(array, own_key, smallest, largest):
    dims = array.shape
    index_at = [jax.random.randint(jax.random.fold_in(own_key, axis), (), 0, dims[axis]) for axis in range(len(dims))]
    array = array.at[tuple(index_at)].set(smallest)
    longest = dims.index(max(dims))
    index_at[longest] = (index_at[longest] + 1) % dims[longest]
    return array.at[tuple(index_at)].set(largest)


def shard_levels(stream_key, shape, cuts, smallest, largest):
    factor_of, own = 1.0, jax.random.fold_in(stream_key, 6)
    for axis_at, blocks in cuts:
        draws = jnp.exp(jax.random.uniform(jax.random.fold_in(own, axis_at), (blocks,), jnp.float32, smallest / len(cuts), largest / len(cuts)))
        factor_of = factor_of * jnp.repeat(draws, shape[axis_at] // blocks).reshape([-1 if axis == axis_at else 1 for axis in range(len(shape))])
    return factor_of


def bell_draw(key, extent, scale, most, pieces=(), kind=jnp.bfloat16):
    values = jax.random.normal(key, extent, jnp.float32) * scale
    if len(pieces) > 0:
        values = shard_levels(key, extent, pieces, -0.22, 0.18) * values
    return jnp.clip(values, min=-most, max=most).astype(kind)


def setup_inputs(seed: int = 0) -> dict:
    seeds = jax.random.split(jax.random.key(seed), 10)
    positions = bell_draw(seeds[0], (BLOCKS, 3, BLOCK), 1.0, 6.0, ((0, 256),), jnp.float32)
    time_bins = set_ends(jax.random.randint(seeds[1], (BLOCKS, BLOCK), 0, BINS), jax.random.fold_in(seeds[1], 1), 0, BINS - 1).astype(jnp.int32)
    home_groups = set_ends(jax.random.randint(seeds[2], (BLOCKS,), 0, GROUPS), jax.random.fold_in(seeds[2], 1), 0, GROUPS - 1).astype(jnp.int32)
    targets = draw_targets(jax.random.fold_in(seeds[9], 71), 0)
    target_groups = set_ends(jax.random.randint(seeds[4], (BLOCKS, TOP), 0, GROUPS), jax.random.fold_in(seeds[4], 1), 0, GROUPS - 1).astype(jnp.int32)
    node_pos = bell_draw(seeds[5], (3, NODES), 1.0, 6.0, ((1, 256),), jnp.float32)
    node_mass = jnp.clip(jnp.exp(math.log(2.0) - 2.3025851 * jax.random.uniform(seeds[6], (NODES,), jnp.float32) ** shard_levels(seeds[6], (NODES,), ((0, 256),), -0.2, 0.2)), 0.2, 2.0)
    node_lists = set_ends(jax.random.randint(seeds[7], (N_DOM * GROUPS, LIST), 0, NODE_DEV * N_SUB), jax.random.fold_in(seeds[7], 1), 0, (NODE_DEV * N_SUB) - 1).astype(jnp.int32)
    list_counts = draw_list_counts(jax.random.fold_in(seeds[9], 71), 0)
    return dict(positions=positions, time_bins=time_bins, home_groups=home_groups, targets=targets, target_groups=target_groups, node_pos=node_pos, node_mass=node_mass, node_lists=node_lists, list_counts=list_counts)


soften_sq = 0.04
gauss_slope = 1.1283791670955126

def short_pull(sink_pos, source_pos, source_mass):
    offset = sink_pos[:, None, :] - source_pos[:, :, None]
    range_sq = lax.optimization_barrier(jnp.sum(offset * offset, axis=0)) + soften_sq
    distance = jnp.sqrt(range_sq)
    scaled = distance * 0.5
    factor = lax.erfc(scaled) + gauss_slope * scaled * jnp.exp(-scaled * scaled)
    weight = source_mass[:, None] * factor / (range_sq * distance)
    return -lax.optimization_barrier(jnp.sum(offset * weight[None, :, :], axis=1))

def reference(positions, time_bins, home_groups, targets, target_groups, node_pos, node_mass, node_lists, list_counts):
    per_domain = BLK_DEV * N_SUB
    node_count = NODE_DEV * N_SUB
    block_ids = jnp.arange(BLOCKS, dtype=jnp.int32)
    home_domain = block_ids // per_domain
    visit_domain = jnp.concatenate([home_domain[:, None], jnp.maximum(targets, 0)], axis=1).astype(jnp.int32)
    visit_group = jnp.concatenate([home_groups[:, None], target_groups], axis=1).astype(jnp.int32)
    visit_alive = jnp.concatenate([jnp.ones((BLOCKS, 1), jnp.float32), (targets >= 0).astype(jnp.float32)], axis=1)
    list_rows = visit_domain * GROUPS + visit_group
    entry_ids = jnp.arange(LIST, dtype=jnp.int32)

    def one_visit(sink_pos, list_row, domain_id, is_alive):
        node_index = node_lists[list_row] + domain_id * node_count
        node_weight = node_mass[node_index] * (entry_ids < list_counts[list_row]).astype(jnp.float32) * is_alive
        return short_pull(sink_pos, node_pos[:, node_index], node_weight)

    def one_block(sink_pos, block_rows, block_domains, block_alive):
        pulls = jax.vmap(one_visit, in_axes=(None, 0, 0, 0))(sink_pos, block_rows, block_domains, block_alive)
        return lax.optimization_barrier(jnp.sum(pulls, axis=0))

    def one_group(operands):
        return jax.vmap(one_block)(*operands)
    grouped = lax.map(one_group, (positions.reshape(BLOCKS // 8, 8, 3, BLOCK), list_rows.reshape(BLOCKS // 8, 8, TOP + 1), visit_domain.reshape(BLOCKS // 8, 8, TOP + 1), visit_alive.reshape(BLOCKS // 8, 8, TOP + 1)))
    summed = grouped.reshape(BLOCKS, 3, BLOCK)
    active = (time_bins <= CUR_BIN).astype(jnp.float32)
    return summed * active[:, None, :]
```

```python
import functools
import jax
import jax.numpy as jnp
from jax import lax
from jax.experimental import pallas as pl
from jax.experimental.pallas import tpu as pltpu
from jax.sharding import PartitionSpec as P

CUR_BIN = 2


def sent_to_all(value, axis):
    length = lax.axis_size(axis)
    return lax.all_to_all(
        jnp.broadcast_to(value[None], (length, *value.shape)), axis, 0, 0, tiled=True
    )


def joined_by_halves(pieces, combine):
    while len(jax.tree.leaves(pieces)[0]) > 1:
        pieces = jax.vmap(combine)(*(pieces[side::2] for side in (0, 1)))
    return pieces[0]


def carried_in(value, axis, combine, identity):
    length, mine = (lax.axis_size(axis), lax.axis_index(axis))
    passed = jnp.arange(length) < mine

    def kept(part, zero, own):
        part = jnp.where(
            passed.reshape(-1, *(1 for _ in own.shape)), part, jnp.asarray(zero, own.dtype)
        )
        return part

    pieces = sent_to_all(value, axis)
    return joined_by_halves(kept(pieces, identity, value), combine)


CHUNK = 32
LOG2E = 1.4426950408889634
SLOPE = 1.1283791670955126
GROUPS = 64
LIST = 256
MIN_STEPS = 2


def pair_sums(xs, node, acc):
    out = list(acc)
    for g in range(CHUNK // 8):
        rows = slice(8 * g, 8 * g + 8)
        d = [xs[c] - jnp.concatenate([node[c][rows]] * 2, axis=1) for c in range(3)]
        s = d[0] * d[0] + (d[1] * d[1] + (d[2] * d[2] + 0.01))
        inv = lax.rsqrt(s)
        e = jnp.exp2(s * (-LOG2E))
        tail = 1.0 - lax.erf(s * inv)
        m = jnp.concatenate([node[3][rows]] * 2, axis=1)
        w = (inv * tail + SLOPE * e) * (inv * inv) * m
        out = [out[c] + d[c] * w for c in range(3)]
    return tuple(out)


def compute_kernel(rows_ref, counts_ref, pos_ref, table_ref, out_ref, cols, first):
    V = rows_ref.shape[0]

    def turn(l, carry):
        t = table_ref[l]
        t = jnp.concatenate([t, t], axis=0)
        cols[l, :, 0:8] = t.T
        return carry
    lax.fori_loop(0, GROUPS, turn, 0, unroll=8)

    def fetch(row, i):
        n = cols[row, CHUNK * i:CHUNK * (i + 1), 0:8]
        return tuple(jnp.broadcast_to(n[:, c:c + 1], (CHUNK, 128)) for c in range(4))

    def prefetch(v):
        row = jnp.maximum(rows_ref[v], 0)
        for c, col in enumerate(fetch(row, 0)):
            first[c] = col
    prefetch(0)

    def visit(v, carry):
        row = rows_ref[v]
        nxt = jnp.minimum(v + 1, V - 1)
        safe = jnp.maximum(row, 0)
        steps = (counts_ref[safe] + (CHUNK - 1)) // CHUNK
        index = jnp.where(row < 0, 0, jnp.clip(steps - (MIN_STEPS - 1), 1, LIST // CHUNK - MIN_STEPS + 1))

        def dead():
            prefetch(nxt)
            out_ref[v] = jnp.zeros((3, 256), jnp.float32)

        def alive(n):
            def run():
                x = pos_ref[v] * 0.5
                xs = [jnp.broadcast_to(x[c:c + 1], (8, 256)) for c in range(3)]
                zero = jnp.zeros((8, 256), jnp.float32)
                acc = (zero, zero, zero)
                acc = pair_sums(xs, tuple(first[c] for c in range(4)), acc)
                prefetch(nxt)
                for i in range(1, n):
                    acc = pair_sums(xs, fetch(safe, i), acc)
                out_ref[v] = jnp.concatenate([jnp.sum(a, axis=0, keepdims=True) for a in acc], axis=0)
            return run
        lax.switch(index, [dead] + [alive(n) for n in range(MIN_STEPS, LIST // CHUNK + 1)])
        return carry
    lax.fori_loop(0, V, visit, 0)


def compute(rows, counts, pos, table):
    V = rows.shape[0]
    return pl.pallas_call(
        compute_kernel,
        out_shape=jax.ShapeDtypeStruct((V, 3, 256), jnp.float32),
        in_specs=[pl.BlockSpec(memory_space=pltpu.SMEM)] * 2 + [pl.BlockSpec(memory_space=pltpu.VMEM)] * 2,
        out_specs=pl.BlockSpec(memory_space=pltpu.VMEM),
        scratch_shapes=[pltpu.VMEM((GROUPS, LIST, 128), jnp.float32), pltpu.VMEM((4, CHUNK, 128), jnp.float32)],
        compiler_params=pltpu.CompilerParams(vmem_limit_bytes=48 * 2**20),
    )(rows, counts, pos, table)


def gather_kernel(lists_ref, counts_ref, nodes_ref, table_ref, tiles, pieces):
    owners = nodes_ref.shape[0]
    per_owner = nodes_ref.shape[2] // 128
    for o in range(owners):
        for j in range(per_owner):
            tiles[o * per_owner + j] = nodes_ref[o, :, 128 * j:128 * (j + 1)]
    for c in range(4):
        left = tiles[:, c, :].T
        for p in range(3):
            part = left.astype(jnp.bfloat16)
            pieces[p, 128 * c:128 * (c + 1), :] = part
            left = left - part.astype(jnp.float32)
    highs = owners * per_owner

    def one_list(l, carry):
        index = lists_ref[pl.ds(l, 1), :]
        high = lax.shift_right_logical(index, 7)
        low = jnp.bitwise_and(index, 127)
        pick = (lax.broadcasted_iota(jnp.int32, (highs, LIST), 0) == high)
        pick = jnp.where(pick, 1.0, 0.0).astype(jnp.bfloat16)
        rows = jnp.zeros((512, LIST), jnp.float32)
        for p in range(3):
            rows = rows + jnp.dot(pieces[p], pick, preferred_element_type=jnp.float32)
        here = lax.broadcasted_iota(jnp.int32, (128, LIST), 0) == low
        valid = lax.broadcasted_iota(jnp.int32, (1, LIST), 1) < counts_ref[l]
        picked = [
            jnp.sum(jnp.where(here, rows[128 * c:128 * (c + 1)], 0.0), axis=0, keepdims=True)
            for c in range(4)
        ]
        table_ref[l] = jnp.concatenate(
            [0.5 * picked[0], 0.5 * picked[1], 0.5 * picked[2], jnp.where(valid, -0.25 * picked[3], 0.0)], axis=0
        )
        return carry
    lax.fori_loop(0, lists_ref.shape[0], one_list, 0)


def gather_lists(lists, counts, nodes):
    owners, _, per = nodes.shape
    return pl.pallas_call(
        gather_kernel,
        out_shape=jax.ShapeDtypeStruct((lists.shape[0], 4, LIST), jnp.float32),
        in_specs=[
            pl.BlockSpec(memory_space=pltpu.VMEM),
            pl.BlockSpec(memory_space=pltpu.SMEM),
            pl.BlockSpec(memory_space=pltpu.VMEM),
        ],
        out_specs=pl.BlockSpec(memory_space=pltpu.VMEM),
        scratch_shapes=[
            pltpu.VMEM((owners * per // 128, 4, 128), jnp.float32),
            pltpu.VMEM((3, 512, owners * per // 128), jnp.bfloat16),
        ],
        compiler_params=pltpu.CompilerParams(vmem_limit_bytes=48 * 2**20),
    )(lists, counts, nodes)

def ranks_within(bucket, usable, bucket_count):
    onehot = (
        (bucket[:, None] == jnp.arange(bucket_count, dtype=jnp.int32)[None, :]) & usable[:, None]
    ).astype(jnp.int32)
    placed = jnp.sum((jnp.cumsum(onehot, axis=0) - onehot) * onehot, axis=1)
    return (placed, jnp.sum(onehot, axis=0))


def owners(slot_index, usable, slot_count):
    matches = (slot_index[None, :] == jnp.arange(slot_count, dtype=jnp.int32)[:, None]) & usable[
        None, :
    ]
    is_filled = jnp.any(matches, axis=1)
    source_row = jnp.sum(
        matches.astype(jnp.int32) * jnp.arange(slot_index.shape[0], dtype=jnp.int32)[None, :],
        axis=1,
    )
    return (source_row, is_filled)


def local(
    positions,
    time_bins,
    home_groups,
    targets,
    target_groups,
    node_pos,
    node_mass,
    node_lists,
    list_counts,
):
    domains = lax.axis_size("dom")
    sharers = lax.axis_size("sub")
    blocks, most_visits = targets.shape
    width = positions.shape[2]
    capacity = max(2, blocks * most_visits // domains)
    nodes = lax.all_gather(jnp.concatenate([node_pos, node_mass[None]], axis=0), "sub")
    share = GROUPS // sharers
    mine = lax.axis_index("sub") * share
    piece = gather_lists(
        lax.dynamic_slice_in_dim(node_lists, mine, share),
        lax.dynamic_slice_in_dim(list_counts, mine, share),
        nodes,
    )
    table = lax.all_gather(piece, "sub", tiled=True)
    home_force = compute(home_groups, list_counts, positions, table)

    def imported(arrived):
        arrived_pos, arrived_group = arrived
        leading = arrived_group.shape
        flat_group = arrived_group.reshape(-1)
        pulled = compute(flat_group, list_counts, arrived_pos.reshape((-1, 3, width)), table)
        return pulled.reshape(leading + (3, width))

    flat_dest = targets.reshape(-1)
    usable = flat_dest >= 0
    safe_dest = jnp.maximum(flat_dest, 0)
    pair_block = jnp.arange(blocks * most_visits, dtype=jnp.int32) // most_visits
    flat_groups = target_groups.reshape(-1)
    within, per_domain = ranks_within(safe_dest, usable, domains)
    first_width = -(-capacity // sharers)
    second_width = -(-2 * capacity // sharers)
    offsets = carried_in(
        per_domain, "sub", lambda earlier, later: earlier + later, jnp.zeros_like(per_domain)
    )
    row_place = offsets[safe_dest] + within
    sharer_of = row_place % sharers
    row_slot = row_place // sharers
    bucket = sharer_of * domains + safe_dest
    within_bucket, _ = ranks_within(bucket, usable, sharers * domains)
    first_slot = bucket * first_width + within_bucket
    source_row, is_filled = owners(first_slot, usable, sharers * domains * first_width)
    out_pos = jnp.where(is_filled[:, None, None], positions[pair_block[source_row]], 0.0).reshape(
        sharers, domains, first_width, 3, width
    )
    out_group = jnp.where(is_filled, flat_groups[source_row], -1).reshape(
        sharers, domains, first_width
    )
    out_slot = jnp.where(is_filled, row_slot[source_row], 0).reshape(sharers, domains, first_width)
    spread_pos, spread_group, spread_slot = (
        lax.all_to_all(out_pos, "sub", split_axis=0, concat_axis=0, tiled=True),
        lax.all_to_all(out_group, "sub", split_axis=0, concat_axis=0, tiled=True),
        lax.all_to_all(out_slot, "sub", split_axis=0, concat_axis=0, tiled=True),
    )
    arrival_dest = (
        jnp.arange(sharers * domains * first_width, dtype=jnp.int32) // first_width % domains
    )
    arrival_group = spread_group.reshape(-1)
    arrival_ok = arrival_group >= 0
    second_index = arrival_dest * second_width + spread_slot.reshape(-1)
    arrival_row, second_filled = owners(second_index, arrival_ok, domains * second_width)
    mid_pos = jnp.where(
        second_filled[:, None, None], spread_pos.reshape(-1, 3, width)[arrival_row], 0.0
    ).reshape(domains, second_width, 3, width)
    mid_group = jnp.where(second_filled, arrival_group[arrival_row], -1).reshape(
        domains, second_width
    )
    computed = imported(
        tuple(lax.all_to_all(a, "dom", split_axis=0, concat_axis=0, tiled=True) for a in (mid_pos, mid_group))
    )
    returned = lax.all_to_all(computed, "dom", split_axis=0, concat_axis=0, tiled=True)
    arrival_force = returned.reshape(domains * second_width, 3, width)[
        jnp.where(arrival_ok, second_index, 0)
    ]
    arrival_force = arrival_force * arrival_ok.astype(jnp.float32)[:, None, None]
    gathered_back = lax.all_to_all(
        arrival_force.reshape(sharers, domains, first_width, 3, width),
        "sub",
        split_axis=0,
        concat_axis=0,
        tiled=True,
    )
    pair_force = gathered_back.reshape(-1, 3, width)[jnp.where(usable, first_slot, 0)]
    pair_force = pair_force * usable.astype(jnp.float32)[:, None, None]
    remote = jnp.sum(pair_force.reshape(blocks, most_visits, 3, width), axis=1)
    active = (time_bins <= CUR_BIN).astype(jnp.float32)
    return (home_force + remote) * active[:, None, :]


def solution(mesh):
    return jax.shard_map(
        local,
        mesh=mesh,
        in_specs=(
            P(("dom", "sub"), None, None),
            P(("dom", "sub"), None),
            P(("dom", "sub")),
            P(("dom", "sub"), None),
            P(("dom", "sub"), None),
            P(None, ("dom", "sub")),
            P(("dom", "sub")),
            P("dom", None),
            P("dom"),
        ),
        out_specs=P(("dom", "sub"), None, None),
        check_vma=False,
    )
```

```python
import jax
import jax.numpy as jnp
from jax import lax
from jax.experimental import pallas as pl
from jax.experimental.pallas import tpu as pltpu
from jax.sharding import PartitionSpec as P

CUR_BIN = 2
CHUNK = 32
LOG2E = 1.4426950408889634
SLOPE = 1.1283791670955126
GROUPS = 64
LIST = 256
MIN_STEPS = 2
N_DOM = 32
N_SUB = 8
TOP = 4
BLK = 64
NODE_DEV = 4096
SHARE = GROUPS // N_SUB
MESH = pl.DeviceIdType.MESH
F32 = jnp.float32
BF16 = jnp.bfloat16


def thirds(value):
    parts = []
    for _ in range(3):
        part = value.astype(BF16)
        parts.append(part)
        value = value - part.astype(F32)
    return parts


def greet(me_dom, me_sub):
    barrier = pltpu.get_barrier_semaphore()
    for p in range(1, N_SUB):
        pl.semaphore_signal(
            barrier, inc=1, device_id={"sub": lax.rem(me_sub + p, N_SUB)}, device_id_type=MESH
        )

    def one(i, carry):
        pl.semaphore_signal(
            barrier, inc=1, device_id={"dom": lax.rem(me_dom + i, N_DOM)}, device_id_type=MESH
        )
        return carry

    lax.fori_loop(1, N_DOM, one, 0)
    return barrier


def to_sub(src, dst, send, recv, peer, slot, mine):
    return pltpu.make_async_remote_copy(
        src_ref=src,
        dst_ref=dst.at[slot],
        send_sem=send.at[peer],
        recv_sem=recv.at[slot],
        device_id={"sub": peer},
        device_id_type=MESH,
    )


def start_sub(src_of, dst, send, recv, me):
    for p in range(1, N_SUB):
        peer = lax.rem(me + p, N_SUB)
        to_sub(src_of(peer), dst, send, recv, peer, me, me).start()


def wait_sub_recv(src_of, dst, send, recv, me):
    for p in range(1, N_SUB):
        peer = lax.rem(me + p, N_SUB)
        to_sub(src_of(peer), dst, send, recv, peer, peer, me).wait_recv()


def wait_sub_send(src_of, dst, send, recv, me):
    for p in range(1, N_SUB):
        peer = lax.rem(me + p, N_SUB)
        to_sub(src_of(peer), dst, send, recv, peer, me, me).wait_send()


def dom_copy(src, dst, send, recv, peer, slot):
    return pltpu.make_async_remote_copy(
        src_ref=src.at[peer],
        dst_ref=dst.at[slot],
        send_sem=send.at[peer],
        recv_sem=recv.at[slot],
        device_id={"dom": peer},
        device_id_type=MESH,
    )


def each_dom(me, act):
    def one(i, carry):
        act(lax.rem(me + i, N_DOM))
        return carry

    lax.fori_loop(1, N_DOM, one, 0)


def build_lists(lists_ref, counts_ref, first_list, tiles, pieces, put):
    highs = tiles.shape[0]
    for c in range(4):
        for p, part in enumerate(thirds(tiles[:, c, :].T)):
            pieces[p, 128 * c : 128 * (c + 1), :] = part

    def one_list(l, carry):
        index = lists_ref[pl.ds(first_list + l, 1), :]
        high = lax.shift_right_logical(index, 7)
        low = jnp.bitwise_and(index, 127)
        pick = lax.broadcasted_iota(jnp.int32, (highs, LIST), 0) == high
        pick = jnp.where(pick, 1.0, 0.0).astype(BF16)
        rows = jnp.zeros((512, LIST), F32)
        for p in range(3):
            rows = rows + jnp.dot(pieces[p], pick, preferred_element_type=F32)
        here = lax.broadcasted_iota(jnp.int32, (128, LIST), 0) == low
        valid = lax.broadcasted_iota(jnp.int32, (1, LIST), 1) < counts_ref[first_list + l]
        picked = [
            jnp.sum(jnp.where(here, rows[128 * c : 128 * (c + 1)], 0.0), axis=0, keepdims=True)
            for c in range(4)
        ]
        mass = jnp.where(valid, -0.25 * picked[3], 0.0)
        put(l, jnp.concatenate([0.5 * picked[0], 0.5 * picked[1], 0.5 * picked[2], mass], axis=0))
        return carry

    lax.fori_loop(0, SHARE, one_list, 0)


def forward_kernel(
    counts_ref,
    tt_ref,
    pos_ref,
    nodes_ref,
    lists_ref,
    table_ref,
    arr_ref,
    codes_ref,
    oh_ref,
    nrecv,
    tiles,
    pieces,
    csend,
    crecv,
    ssend,
    srecv,
    mid,
    arr,
    trecv,
    n_send,
    n_recv,
    c_send,
    c_recv,
    s_send,
    s_recv,
    t_send,
    t_recv,
    d_send,
    d_recv,
):
    me_dom = lax.axis_index("dom")
    me = lax.axis_index("sub")
    barrier = greet(me_dom, me)

    dom_ids = lax.broadcasted_iota(jnp.int32, (N_DOM, 128), 0)
    wants = [dom_ids == tt_ref[j : j + 1, :] for j in range(TOP)]
    ones_of = [jnp.where(w, 1.0, 0.0) for w in wants]
    csend[...] = (ones_of[0] + ones_of[1]) + (ones_of[2] + ones_of[3])
    pl.semaphore_wait(barrier, N_SUB - 1 + N_DOM - 1)
    start_sub(lambda peer: csend, crecv, c_send, c_recv, me)
    start_sub(lambda peer: nodes_ref, nrecv, n_send, n_recv, me)

    earlier = lax.broadcasted_iota(jnp.int32, (128, 128), 0) < lax.broadcasted_iota(
        jnp.int32, (128, 128), 1
    )
    earlier = jnp.where(earlier, 1.0, 0.0).astype(BF16)
    full = jnp.ones((128, 128), BF16)
    within = [jnp.dot(o.astype(BF16), earlier, preferred_element_type=F32) for o in ones_of]
    total = [jnp.dot(o.astype(BF16), full, preferred_element_type=F32) for o in ones_of]
    pos_parts = [thirds(pos_ref[:, c, :]) for c in range(3)]
    wait_sub_recv(lambda peer: csend, crecv, c_send, c_recv, me)
    before = jnp.zeros((N_DOM, 128), F32)
    for p in range(1, N_SUB):
        peer = lax.rem(me + p, N_SUB)
        before = before + jnp.where(peer < me, 1.0, 0.0) * crecv[peer]
    base = jnp.dot(before.astype(BF16), full, preferred_element_type=F32)
    sharer, turn = [], []
    for j in range(TOP):
        place = (base + within[j]).astype(jnp.int32)
        base = base + total[j]
        sharer.append(jnp.bitwise_and(place, N_SUB - 1))
        turn.append(lax.shift_right_logical(place, 3))
    for t in range(N_SUB):
        hot = jnp.zeros((N_DOM, 128), F32)
        code = jnp.zeros((N_DOM, 128), F32)
        for j in range(TOP):
            mine = wants[j] & (sharer[j] == t)
            hot = jnp.where(mine, 1.0, hot)
            mark = tt_ref[TOP + j : TOP + j + 1, :] + (1 + GROUPS * turn[j])
            code = jnp.where(mine, mark.astype(F32), code)
        oh_ref[N_DOM * t : N_DOM * (t + 1), :] = hot.astype(BF16)
        ssend[t, :, 768:896] = jnp.dot(code.astype(BF16), full, preferred_element_type=F32)
    picks = oh_ref[:, 0:BLK]
    for c in range(3):
        rows = jnp.zeros((N_SUB * N_DOM, 256), F32)
        for part in pos_parts[c]:
            rows = rows + jnp.dot(picks, part, preferred_element_type=F32)
        for t in range(N_SUB):
            ssend[t, :, 256 * c : 256 * (c + 1)] = rows[N_DOM * t : N_DOM * (t + 1)]
    start_sub(lambda peer: ssend.at[peer], srecv, s_send, s_recv, me)
    srecv[me] = ssend[me]

    nrecv[me] = nodes_ref[...]
    wait_sub_recv(lambda peer: nodes_ref, nrecv, n_send, n_recv, me)

    def owner_tiles(o, carry):
        for j in range(NODE_DEV // 128):
            tiles[o * (NODE_DEV // 128) + j] = nrecv[o, :, 128 * j : 128 * (j + 1)]
        return carry

    lax.fori_loop(0, N_SUB, owner_tiles, 0)

    def put(l, value):
        trecv[me, l] = value

    build_lists(lists_ref, counts_ref, me * SHARE, tiles, pieces, put)
    start_sub(lambda peer: trecv.at[me], trecv, t_send, t_recv, me)

    wait_sub_recv(lambda peer: ssend.at[peer], srecv, s_send, s_recv, me)
    for k in range(2):
        for q in range(7):
            value = jnp.zeros((N_DOM, 128), F32)
            for src in range(N_SUB):
                code = srecv[src, :, 768:896]
                mine = (code > GROUPS + 0.5) if k else ((code > 0.5) & (code < GROUPS + 0.5))
                if q == 6:
                    value = jnp.where(mine, code - float(GROUPS * k), value)
                else:
                    value = jnp.where(mine, srecv[src, :, 128 * q : 128 * (q + 1)], value)
            mid[:, k, q, :] = value
        mid[:, k, 7, :] = jnp.zeros((N_DOM, 128), F32)
    each_dom(me_dom, lambda peer: dom_copy(mid, arr, d_send, d_recv, peer, me_dom).start())
    arr[me_dom] = jnp.zeros((2, 8, 128), F32)
    for src in range(N_SUB):
        codes_ref[src] = srecv[src, :, 768:896]

    wait_sub_recv(lambda peer: trecv.at[me], trecv, t_send, t_recv, me)
    for src in range(N_SUB):
        table_ref[SHARE * src : SHARE * (src + 1)] = trecv[src]
    each_dom(me_dom, lambda peer: dom_copy(mid, arr, d_send, d_recv, peer, peer).wait_recv())
    for k in range(2):
        arr_ref[:, k] = arr[:, k]

    wait_sub_send(lambda peer: csend, crecv, c_send, c_recv, me)
    wait_sub_send(lambda peer: nodes_ref, nrecv, n_send, n_recv, me)
    wait_sub_send(lambda peer: ssend.at[peer], srecv, s_send, s_recv, me)
    wait_sub_send(lambda peer: trecv.at[me], trecv, t_send, t_recv, me)
    each_dom(me_dom, lambda peer: dom_copy(mid, arr, d_send, d_recv, peer, me_dom).wait_send())


def forward(counts, tt, pos, nodes, lists):
    vmem = pl.BlockSpec(memory_space=pltpu.VMEM)
    dma = pltpu.SemaphoreType.DMA
    return pl.pallas_call(
        forward_kernel,
        out_shape=(
            jax.ShapeDtypeStruct((GROUPS, 4, LIST), F32),
            jax.ShapeDtypeStruct((N_DOM, 2, 8, 128), F32),
            jax.ShapeDtypeStruct((N_SUB, N_DOM, 128), F32),
            jax.ShapeDtypeStruct((N_SUB * N_DOM, 128), BF16),
        ),
        in_specs=[pl.BlockSpec(memory_space=pltpu.SMEM)] + [vmem] * 4,
        out_specs=(vmem,) * 4,
        scratch_shapes=[
            pltpu.VMEM((N_SUB, 4, NODE_DEV), F32),
            pltpu.VMEM((N_SUB * NODE_DEV // 128, 4, 128), F32),
            pltpu.VMEM((3, 512, N_SUB * NODE_DEV // 128), BF16),
            pltpu.VMEM((N_DOM, 128), F32),
            pltpu.VMEM((N_SUB, N_DOM, 128), F32),
            pltpu.VMEM((N_SUB, N_DOM, 896), F32),
            pltpu.VMEM((N_SUB, N_DOM, 896), F32),
            pltpu.VMEM((N_DOM, 2, 8, 128), F32),
            pltpu.VMEM((N_DOM, 2, 8, 128), F32),
            pltpu.VMEM((N_SUB, SHARE, 4, LIST), F32),
        ]
        + [dma((N_SUB,))] * 8
        + [dma((N_DOM,))] * 2,
        compiler_params=pltpu.CompilerParams(
            collective_id=0, has_side_effects=True, vmem_limit_bytes=48 * 2**20
        ),
    )(counts, tt, pos, nodes, lists)


def pair_sums(xs, node, acc):
    out = list(acc)
    for g in range(CHUNK // 8):
        rows = slice(8 * g, 8 * g + 8)
        cols = [jnp.concatenate([node[c][rows]] * 2, axis=1) for c in range(4)]
        d = [xs[c] - cols[c] for c in range(3)]
        s = d[0] * d[0] + (d[1] * d[1] + (d[2] * d[2] + 0.01))
        inv = lax.rsqrt(s)
        e = jnp.exp2(s * (-LOG2E))
        tail = 1.0 - lax.erf(s * inv)
        w = (inv * tail + SLOPE * e) * (inv * inv) * cols[3]
        out = [out[c] + d[c] * w for c in range(3)]
    return tuple(out)


def turn_tables(table_ref, cols):
    def one(l, carry):
        t = table_ref[l]
        t = jnp.concatenate([t, t], axis=0)
        cols[l, :, 0:8] = t.T
        return carry

    lax.fori_loop(0, GROUPS, one, 0, unroll=8)


def fetch(cols, row, i):
    n = cols[row, CHUNK * i : CHUNK * (i + 1), 0:8]
    return tuple(jnp.broadcast_to(n[:, c : c + 1], (CHUNK, 128)) for c in range(4))


def halves(rows):
    return [
        jnp.concatenate([jnp.broadcast_to(rows[2 * c + h], (8, 128)) for h in range(2)], axis=1)
        for c in range(3)
    ]


def import_kernel(rows_ref, counts_ref, arr_ref, table_ref, out_ref, cols, first):
    visits = rows_ref.shape[0]
    turn_tables(table_ref, cols)

    def prefetch(v):
        row = jnp.maximum(rows_ref[v], 0)
        for c, col in enumerate(fetch(cols, row, 0)):
            first[c] = col

    prefetch(0)

    def visit(v, carry):
        row = rows_ref[v]
        nxt = jnp.minimum(v + 1, visits - 1)
        safe = jnp.maximum(row, 0)
        steps = (counts_ref[safe] + (CHUNK - 1)) // CHUNK
        index = jnp.where(
            row < 0, 0, jnp.clip(steps - (MIN_STEPS - 1), 1, LIST // CHUNK - MIN_STEPS + 1)
        )

        def dead():
            prefetch(nxt)
            out_ref[v] = jnp.zeros((8, 128), F32)

        def alive(n):
            def run():
                x = arr_ref[v] * 0.5
                xs = halves([x[q : q + 1] for q in range(6)])
                zero = jnp.zeros((8, 256), F32)
                acc = pair_sums(xs, tuple(first[c] for c in range(4)), (zero, zero, zero))
                prefetch(nxt)
                for i in range(1, n):
                    acc = pair_sums(xs, fetch(cols, safe, i), acc)
                sums = [jnp.sum(a, axis=0, keepdims=True) for a in acc]
                rows = [sums[c][:, 128 * h : 128 * (h + 1)] for c in range(3) for h in range(2)]
                out_ref[v] = jnp.concatenate(rows + [jnp.zeros((2, 128), F32)], axis=0)

            return run

        lax.switch(index, [dead] + [alive(n) for n in range(MIN_STEPS, LIST // CHUNK + 1)])
        return carry

    lax.fori_loop(0, visits, visit, 0)


def import_pulls(rows, counts, arrived, table):
    smem = pl.BlockSpec(memory_space=pltpu.SMEM)
    vmem = pl.BlockSpec(memory_space=pltpu.VMEM)
    return pl.pallas_call(
        import_kernel,
        out_shape=jax.ShapeDtypeStruct(arrived.shape, F32),
        in_specs=[smem, smem, vmem, vmem],
        out_specs=vmem,
        scratch_shapes=[pltpu.VMEM((GROUPS, LIST, 128), F32), pltpu.VMEM((4, CHUNK, 128), F32)],
        compiler_params=pltpu.CompilerParams(vmem_limit_bytes=48 * 2**20),
    )(rows, counts, arrived, table)


def return_kernel(
    groups_ref,
    pos_ref,
    bins_ref,
    table_ref,
    pulls_ref,
    codes_ref,
    oh_ref,
    out_ref,
    cols,
    first,
    home,
    ret,
    bsend,
    brecv,
    d_send,
    d_recv,
    b_send,
    b_recv,
):
    me_dom = lax.axis_index("dom")
    me = lax.axis_index("sub")
    barrier = greet(me_dom, me)
    turn_tables(table_ref, cols)
    ret[me_dom] = jnp.zeros((2, 8, 128), F32)
    pl.semaphore_wait(barrier, N_SUB - 1 + N_DOM - 1)
    each_dom(me_dom, lambda peer: dom_copy(pulls_ref, ret, d_send, d_recv, peer, me_dom).start())

    def prefetch(v):
        for c, col in enumerate(fetch(cols, groups_ref[v], 0)):
            first[c] = col

    def home_block(v, carry):
        x = pos_ref[v] * 0.5
        xs = [jnp.broadcast_to(x[c : c + 1], (8, 256)) for c in range(3)]
        zero = jnp.zeros((8, 256), F32)
        acc = pair_sums(xs, tuple(first[c] for c in range(4)), (zero, zero, zero))
        prefetch(jnp.minimum(v + 1, BLK - 1))
        for i in range(1, LIST // CHUNK):
            acc = pair_sums(xs, fetch(cols, groups_ref[v], i), acc)
        for c in range(3):
            home[c, pl.ds(v, 1), :] = jnp.sum(acc[c], axis=0, keepdims=True)
        return carry

    prefetch(0)
    lax.fori_loop(0, EARLY, home_block, 0)

    each_dom(me_dom, lambda peer: dom_copy(pulls_ref, ret, d_send, d_recv, peer, peer).wait_recv())
    for q in range(6):
        low, high = ret[:, 0, q, :], ret[:, 1, q, :]
        for t in range(N_SUB):
            code = codes_ref[t]
            value = jnp.where(code > GROUPS + 0.5, high, jnp.where(code > 0.5, low, 0.0))
            bsend[t, :, 128 * q : 128 * (q + 1)] = value
    start_sub(lambda peer: bsend.at[peer], brecv, b_send, b_recv, me)
    brecv[me] = bsend[me]

    lax.fori_loop(EARLY, BLK, home_block, 0)

    wait_sub_recv(lambda peer: bsend.at[peer], brecv, b_send, b_recv, me)
    active = jnp.where(bins_ref[...] <= CUR_BIN, 1.0, 0.0)
    picks = oh_ref[...]
    for c in range(3):
        back = jnp.concatenate([brecv[t, :, 256 * c : 256 * (c + 1)] for t in range(N_SUB)], axis=0)
        total = home[c]
        for part in thirds(back):
            got = lax.dot_general(
                picks, part, (((0,), (0,)), ((), ())), preferred_element_type=F32
            )
            total = total + got[0:BLK]
        out_ref[:, c, :] = total * active

    each_dom(me_dom, lambda peer: dom_copy(pulls_ref, ret, d_send, d_recv, peer, me_dom).wait_send())
    wait_sub_send(lambda peer: bsend.at[peer], brecv, b_send, b_recv, me)


EARLY = 24


def finish(groups, pos, bins, table, pulls, codes, oh):
    vmem = pl.BlockSpec(memory_space=pltpu.VMEM)
    dma = pltpu.SemaphoreType.DMA
    return pl.pallas_call(
        return_kernel,
        out_shape=jax.ShapeDtypeStruct((BLK, 3, 256), F32),
        in_specs=[pl.BlockSpec(memory_space=pltpu.SMEM)] + [vmem] * 6,
        out_specs=vmem,
        scratch_shapes=[
            pltpu.VMEM((GROUPS, LIST, 128), F32),
            pltpu.VMEM((4, CHUNK, 128), F32),
            pltpu.VMEM((3, BLK, 256), F32),
            pltpu.VMEM((N_DOM, 2, 8, 128), F32),
            pltpu.VMEM((N_SUB, N_DOM, 768), F32),
            pltpu.VMEM((N_SUB, N_DOM, 768), F32),
            dma((N_DOM,)),
            dma((N_DOM,)),
            dma((N_SUB,)),
            dma((N_SUB,)),
        ],
        compiler_params=pltpu.CompilerParams(
            collective_id=1, has_side_effects=True, vmem_limit_bytes=48 * 2**20
        ),
    )(groups, pos, bins, table, pulls, codes, oh)


def local(
    positions,
    time_bins,
    home_groups,
    targets,
    target_groups,
    node_pos,
    node_mass,
    node_lists,
    list_counts,
):
    tt = jnp.pad(
        jnp.concatenate([targets, target_groups], axis=1).T,
        ((0, 0), (0, 128 - BLK)),
        constant_values=-1,
    )
    nodes = jnp.concatenate([node_pos, node_mass[None]], axis=0)
    table, arrived, codes, oh = forward(list_counts, tt, positions, nodes, node_lists)
    arrived = arrived.reshape(2 * N_DOM, 8, 128)
    rows = arrived[:, 6, 0].astype(jnp.int32) - 1
    pulls = import_pulls(rows, list_counts, arrived, table)
    return finish(
        home_groups, positions, time_bins, table, pulls.reshape(N_DOM, 2, 8, 128), codes, oh
    )


def solution(mesh):
    return jax.shard_map(
        local,
        mesh=mesh,
        in_specs=(
            P(("dom", "sub"), None, None),
            P(("dom", "sub"), None),
            P(("dom", "sub")),
            P(("dom", "sub"), None),
            P(("dom", "sub"), None),
            P(None, ("dom", "sub")),
            P(("dom", "sub")),
            P("dom", None),
            P("dom"),
        ),
        out_specs=P(("dom", "sub"), None, None),
        check_vma=False,
    )
```

```python
import jax
import jax.numpy as jnp
from jax import lax
from jax.experimental import pallas as pl
from jax.experimental.pallas import tpu as pltpu
from jax.sharding import PartitionSpec as P

CUR_BIN = 2
LOG2E = 1.4426950408889634
SLOPE = 1.1283791670955126
GROUPS = 64
LIST = 256
N_DOM = 32
N_SUB = 8
TOP = 4
BLK = 64
NODE_DEV = 4096
FIRST = 8
SECOND = 28
SHARE = GROUPS // N_SUB
MESH = pl.DeviceIdType.MESH
F32 = jnp.float32
BF16 = jnp.bfloat16


def thirds(value):
    parts = []
    for _ in range(3):
        part = value.astype(BF16)
        parts.append(part)
        value = value - part.astype(F32)
    return parts


def greet(me_dom, me_sub):
    barrier = pltpu.get_barrier_semaphore()
    for p in range(1, N_SUB):
        pl.semaphore_signal(
            barrier, inc=1, device_id={"sub": lax.rem(me_sub + p, N_SUB)}, device_id_type=MESH
        )

    def one(i, carry):
        pl.semaphore_signal(
            barrier, inc=1, device_id={"dom": lax.rem(me_dom + i, N_DOM)}, device_id_type=MESH
        )
        return carry

    lax.fori_loop(1, N_DOM, one, 0)
    return barrier


def to_sub(src, dst, send, recv, peer, slot, mine):
    return pltpu.make_async_remote_copy(
        src_ref=src,
        dst_ref=dst.at[slot],
        send_sem=send.at[peer],
        recv_sem=recv.at[slot],
        device_id={"sub": peer},
        device_id_type=MESH,
    )


def start_sub(src_of, dst, send, recv, me):
    for p in range(1, N_SUB):
        peer = lax.rem(me + p, N_SUB)
        to_sub(src_of(peer), dst, send, recv, peer, me, me).start()


def wait_sub_recv(src_of, dst, send, recv, me):
    for p in range(1, N_SUB):
        peer = lax.rem(me + p, N_SUB)
        to_sub(src_of(peer), dst, send, recv, peer, peer, me).wait_recv()


def wait_sub_send(src_of, dst, send, recv, me):
    for p in range(1, N_SUB):
        peer = lax.rem(me + p, N_SUB)
        to_sub(src_of(peer), dst, send, recv, peer, me, me).wait_send()


def dom_copy(src, dst, send, recv, peer, slot):
    return pltpu.make_async_remote_copy(
        src_ref=src.at[peer],
        dst_ref=dst.at[slot],
        send_sem=send.at[peer],
        recv_sem=recv.at[slot],
        device_id={"dom": peer},
        device_id_type=MESH,
    )


def each_dom(me, act):
    def one(i, carry):
        act(lax.rem(me + i, N_DOM))
        return carry

    lax.fori_loop(1, N_DOM, one, 0)


def build_lists(lists_ref, counts_ref, first_list, tiles, pieces, put):
    highs = tiles.shape[0]
    for c in range(4):
        for p, part in enumerate(thirds(tiles[:, c, :].T)):
            pieces[p, 128 * c : 128 * (c + 1), :] = part

    def one_list(l, carry):
        index = lists_ref[pl.ds(first_list + l, 1), :]
        high = lax.shift_right_logical(index, 7)
        low = jnp.bitwise_and(index, 127)
        pick = lax.broadcasted_iota(jnp.int32, (highs, LIST), 0) == high
        pick = jnp.where(pick, 1.0, 0.0).astype(BF16)
        rows = jnp.zeros((512, LIST), F32)
        for p in range(3):
            rows = rows + jnp.dot(pieces[p], pick, preferred_element_type=F32)
        here = lax.broadcasted_iota(jnp.int32, (128, LIST), 0) == low
        valid = lax.broadcasted_iota(jnp.int32, (1, LIST), 1) < counts_ref[first_list + l]
        picked = [
            jnp.sum(jnp.where(here, rows[128 * c : 128 * (c + 1)], 0.0), axis=0, keepdims=True)
            for c in range(4)
        ]
        mass = jnp.where(valid, -0.25 * picked[3], 0.0)
        put(l, jnp.concatenate([0.5 * picked[0], 0.5 * picked[1], 0.5 * picked[2], mass], axis=0))
        return carry

    lax.fori_loop(0, SHARE, one_list, 0)


def back_copy(src, dst, k, send, recv, peer, slot):
    return pltpu.make_async_remote_copy(
        src_ref=src.at[k, peer],
        dst_ref=dst.at[slot, k],
        send_sem=send.at[peer],
        recv_sem=recv.at[slot],
        device_id={"dom": peer},
        device_id_type=MESH,
    )


def spread_tables(lists, wide):
    pick = lax.broadcasted_iota(jnp.int32, (8, 256), 0)
    side = jnp.where(lax.broadcasted_iota(jnp.int32, (8, 256), 1) < 128, 2, 5)
    pick = jnp.where((pick >= side) & (pick < side + 3), 1.0, 0.0).astype(BF16)

    def one(o, carry):
        for l in range(SHARE):
            t = lists[o, l]
            rows = [t[0:1], t[1:2]]
            for c in (2, 3):
                rows += [part.astype(F32) for part in thirds(t[c : c + 1])]
            t = jnp.concatenate(rows, axis=0).T
            for c in range(2):
                wide[o * SHARE + l, c] = jnp.broadcast_to(t[:, c : c + 1], (LIST, 128))
            both = jnp.dot(t.astype(BF16), pick, preferred_element_type=F32)
            for c in range(2):
                wide[o * SHARE + l, 2 + c] = both[:, 128 * c : 128 * (c + 1)]
        return carry

    lax.fori_loop(0, N_SUB, one, 0)


def visit_sums(wide, row, rows, held):
    sinks = [jnp.broadcast_to(r * 0.5, (8, 128)) for r in rows]
    acc = [jnp.zeros((8, 128), F32) for _ in range(6)]
    for g in range(LIST // 8):
        node = [wide[row, c, 8 * g : 8 * (g + 1), :] for c in range(4)]
        for h in range(2):
            d = [sinks[2 * c + h] - node[c] for c in range(3)]
            s = d[0] * d[0] + (d[1] * d[1] + (d[2] * d[2] + 0.01))
            inv = lax.rsqrt(s)
            e = jnp.exp2(s * (-LOG2E))
            tail = 1.0 - lax.erf(s * inv)
            w = (inv * tail + SLOPE * e) * (inv * inv) * node[3]
            for c in range(3):
                acc[2 * c + h] = acc[2 * c + h] + d[c] * w
    for q in range(6):
        held[q] = acc[q]


def whole_kernel(
    counts_ref,
    groups_ref,
    tt_ref,
    pos_ref,
    nodes_ref,
    lists_ref,
    bins_ref,
    out_ref,
    nrecv,
    tiles,
    pieces,
    csend,
    crecv,
    ssend,
    srecv,
    mid,
    arr,
    trecv,
    hots,
    wide,
    held,
    home,
    pulls,
    ret,
    bsend,
    brecv,
    picked_rows,
    rows_ref,
    rows_sem,
    n_send,
    n_recv,
    c_send,
    c_recv,
    s_send,
    s_recv,
    t_send,
    t_recv,
    b_send,
    b_recv,
    d_send,
    d_recv,
    low_send,
    low_recv,
    high_send,
    high_recv,
):
    me_dom = lax.axis_index("dom")
    me = lax.axis_index("sub")
    barrier = greet(me_dom, me)

    dom_ids = lax.broadcasted_iota(jnp.int32, (N_DOM, 128), 0)
    wants = [dom_ids == tt_ref[j : j + 1, :] for j in range(TOP)]
    ones_of = [jnp.where(w, 1.0, 0.0) for w in wants]
    csend[...] = (ones_of[0] + ones_of[1]) + (ones_of[2] + ones_of[3])
    earlier = lax.broadcasted_iota(jnp.int32, (128, 128), 0) < lax.broadcasted_iota(
        jnp.int32, (128, 128), 1
    )
    earlier = jnp.where(earlier, 1.0, 0.0).astype(BF16)
    full = jnp.ones((128, 128), BF16)
    within = [jnp.dot(o.astype(BF16), earlier, preferred_element_type=F32) for o in ones_of]
    total = [jnp.dot(o.astype(BF16), full, preferred_element_type=F32) for o in ones_of]
    pos_parts = [thirds(pos_ref[c]) for c in range(3)]
    held[...] = jnp.zeros((6, 8, 128), F32)
    pl.semaphore_wait(barrier, N_SUB - 1 + N_DOM - 1)
    start_sub(lambda peer: csend, crecv, c_send, c_recv, me)
    start_sub(lambda peer: nodes_ref, nrecv, n_send, n_recv, me)
    wait_sub_recv(lambda peer: csend, crecv, c_send, c_recv, me)
    before = jnp.zeros((N_DOM, 128), F32)
    for p in range(1, N_SUB):
        peer = lax.rem(me + p, N_SUB)
        before = before + jnp.where(peer < me, 1.0, 0.0) * crecv[peer]
    base = jnp.dot(before.astype(BF16), full, preferred_element_type=F32)
    sharer, turn = [], []
    for j in range(TOP):
        place = (base + within[j]).astype(jnp.int32)
        base = base + total[j]
        sharer.append(jnp.bitwise_and(place, N_SUB - 1))
        turn.append(lax.shift_right_logical(place, 3))
    for t in range(N_SUB):
        hot = jnp.zeros((N_DOM, 128), F32)
        code = jnp.zeros((N_DOM, 128), F32)
        for j in range(TOP):
            mine = wants[j] & (sharer[j] == t)
            hot = jnp.where(mine, 1.0, hot)
            mark = tt_ref[TOP + j : TOP + j + 1, :] + (1 + GROUPS * turn[j])
            code = jnp.where(mine, mark.astype(F32), code)
        hots[N_DOM * t : N_DOM * (t + 1), :] = hot.astype(BF16)
        ssend[t, :, 768:896] = jnp.dot(code.astype(BF16), full, preferred_element_type=F32)
    picks = hots[:, 0:BLK]
    for c in range(3):
        rows = jnp.zeros((N_SUB * N_DOM, 256), F32)
        for part in pos_parts[c]:
            rows = rows + jnp.dot(picks, part, preferred_element_type=F32)
        for t in range(N_SUB):
            ssend[t, :, 256 * c : 256 * (c + 1)] = rows[N_DOM * t : N_DOM * (t + 1)]
    start_sub(lambda peer: ssend.at[peer], srecv, s_send, s_recv, me)
    srecv[me] = ssend[me]

    nrecv[me] = nodes_ref[...]
    wait_sub_recv(lambda peer: nodes_ref, nrecv, n_send, n_recv, me)

    def owner_tiles(o, carry):
        for j in range(NODE_DEV // 128):
            tiles[o * (NODE_DEV // 128) + j] = nrecv[o, :, 128 * j : 128 * (j + 1)]
        return carry

    lax.fori_loop(0, N_SUB, owner_tiles, 0)

    def put(l, value):
        trecv[me, l] = value

    build_lists(lists_ref, counts_ref, me * SHARE, tiles, pieces, put)
    start_sub(lambda peer: trecv.at[me], trecv, t_send, t_recv, me)

    wait_sub_recv(lambda peer: ssend.at[peer], srecv, s_send, s_recv, me)
    for k in range(2):
        for q in range(7):
            value = jnp.zeros((N_DOM, 128), F32)
            for src in range(N_SUB):
                code = srecv[src, :, 768:896]
                mine = (code > GROUPS + 0.5) if k else ((code > 0.5) & (code < GROUPS + 0.5))
                if q == 6:
                    value = jnp.where(mine, code - float(GROUPS * k), value)
                else:
                    value = jnp.where(mine, srecv[src, :, 128 * q : 128 * (q + 1)], value)
            mid[:, k, q, :] = value
        mid[:, k, 7, :] = jnp.zeros((N_DOM, 128), F32)
    each_dom(me_dom, lambda peer: dom_copy(mid, arr, d_send, d_recv, peer, me_dom).start())
    arr[me_dom] = jnp.zeros((2, 8, 128), F32)
    ret[me_dom] = jnp.zeros((2, 8, 128), F32)

    wait_sub_recv(lambda peer: trecv.at[me], trecv, t_send, t_recv, me)
    spread_tables(trecv, wide)

    def home_rows(v):
        rows = [pos_ref[c, pl.ds(v, 1), :] for c in range(3)]
        return [r[:, 128 * h : 128 * (h + 1)] for r in rows for h in range(2)]

    def home_flush(v):
        for c in range(3):
            parts = [jnp.sum(held[2 * c + h], axis=0, keepdims=True) for h in range(2)]
            home[c, pl.ds(v, 1), :] = jnp.concatenate(parts, axis=1)

    def home_blocks(low, high):
        def one(v, carry):
            home_flush(jnp.maximum(v - 1, low))
            visit_sums(wide, groups_ref[v], home_rows(v), held)
            return carry

        lax.fori_loop(low, high, one, 0)
        home_flush(high - 1)

    home_blocks(0, FIRST)
    each_dom(me_dom, lambda peer: dom_copy(mid, arr, d_send, d_recv, peer, peer).wait_recv())
    diagonal = dom_ids == lax.broadcasted_iota(jnp.int32, (N_DOM, 128), 1)
    marks = [
        jnp.sum(jnp.where(diagonal, arr[:, k, 6, :], 0.0), axis=0, keepdims=True) for k in range(2)
    ]
    marks = jnp.concatenate(marks + [jnp.zeros((6, 128), F32)], axis=0)
    picked_rows[...] = jnp.clip(marks.astype(jnp.int32) - 1, 0, GROUPS - 1)
    to_scalars = pltpu.make_async_copy(picked_rows, rows_ref, rows_sem)
    to_scalars.start()
    to_scalars.wait()

    def imports(k, send, recv):
        def flush(i):
            rows = [jnp.sum(held[q], axis=0, keepdims=True) for q in range(6)]
            rows.append(jnp.zeros((2, 128), F32))
            pulls[k, lax.rem(me_dom + i, N_DOM)] = jnp.concatenate(rows, axis=0)

        def one(i, carry):
            flush(jnp.maximum(i - 1, 1))
            peer = lax.rem(me_dom + i, N_DOM)
            row = rows_ref[k, peer]
            visit_sums(wide, row, [arr[peer, k, q : q + 1, :] for q in range(6)], held)
            return carry

        lax.fori_loop(1, N_DOM, one, 0)
        flush(N_DOM - 1)
        each_dom(me_dom, lambda peer: back_copy(pulls, ret, k, send, recv, peer, me_dom).start())

    imports(0, low_send, low_recv)
    imports(1, high_send, high_recv)

    home_blocks(FIRST, SECOND)

    for k, send, recv in ((0, low_send, low_recv), (1, high_send, high_recv)):
        each_dom(me_dom, lambda peer: back_copy(pulls, ret, k, send, recv, peer, peer).wait_recv())
    for q in range(6):
        low, high = ret[:, 0, q, :], ret[:, 1, q, :]
        for t in range(N_SUB):
            code = srecv[t, :, 768:896]
            value = jnp.where(code > GROUPS + 0.5, high, jnp.where(code > 0.5, low, 0.0))
            bsend[t, :, 128 * q : 128 * (q + 1)] = value
    start_sub(lambda peer: bsend.at[peer], brecv, b_send, b_recv, me)
    brecv[me] = bsend[me]

    home_blocks(SECOND, BLK)

    wait_sub_recv(lambda peer: bsend.at[peer], brecv, b_send, b_recv, me)
    active = jnp.where(bins_ref[...] <= CUR_BIN, 1.0, 0.0)
    picks = hots[...]
    for c in range(3):
        back = jnp.concatenate([brecv[t, :, 256 * c : 256 * (c + 1)] for t in range(N_SUB)], axis=0)
        total = home[c]
        for part in thirds(back):
            got = lax.dot_general(
                picks, part, (((0,), (0,)), ((), ())), preferred_element_type=F32
            )
            total = total + got[0:BLK]
        out_ref[c] = total * active

    wait_sub_send(lambda peer: csend, crecv, c_send, c_recv, me)
    wait_sub_send(lambda peer: nodes_ref, nrecv, n_send, n_recv, me)
    wait_sub_send(lambda peer: ssend.at[peer], srecv, s_send, s_recv, me)
    wait_sub_send(lambda peer: trecv.at[me], trecv, t_send, t_recv, me)
    wait_sub_send(lambda peer: bsend.at[peer], brecv, b_send, b_recv, me)
    each_dom(me_dom, lambda peer: dom_copy(mid, arr, d_send, d_recv, peer, me_dom).wait_send())
    for k, send, recv in ((0, low_send, low_recv), (1, high_send, high_recv)):
        each_dom(me_dom, lambda peer: back_copy(pulls, ret, k, send, recv, peer, me_dom).wait_send())


def whole(counts, groups, tt, pos, nodes, lists, bins):
    smem = pl.BlockSpec(memory_space=pltpu.SMEM)
    vmem = pl.BlockSpec(memory_space=pltpu.VMEM)
    dma = pltpu.SemaphoreType.DMA
    return pl.pallas_call(
        whole_kernel,
        out_shape=jax.ShapeDtypeStruct((3, BLK, 256), F32),
        in_specs=[smem] * 2 + [vmem] * 5,
        out_specs=vmem,
        scratch_shapes=[
            pltpu.VMEM((N_SUB, 4, NODE_DEV), F32),
            pltpu.VMEM((N_SUB * NODE_DEV // 128, 4, 128), F32),
            pltpu.VMEM((3, 512, N_SUB * NODE_DEV // 128), BF16),
            pltpu.VMEM((N_DOM, 128), F32),
            pltpu.VMEM((N_SUB, N_DOM, 128), F32),
            pltpu.VMEM((N_SUB, N_DOM, 896), F32),
            pltpu.VMEM((N_SUB, N_DOM, 896), F32),
            pltpu.VMEM((N_DOM, 2, 8, 128), F32),
            pltpu.VMEM((N_DOM, 2, 8, 128), F32),
            pltpu.VMEM((N_SUB, SHARE, 4, LIST), F32),
            pltpu.VMEM((N_SUB * N_DOM, 128), BF16),
            pltpu.VMEM((GROUPS, 4, LIST, 128), F32),
            pltpu.VMEM((6, 8, 128), F32),
            pltpu.VMEM((3, BLK, 256), F32),
            pltpu.VMEM((2, N_DOM, 8, 128), F32),
            pltpu.VMEM((N_DOM, 2, 8, 128), F32),
            pltpu.VMEM((N_SUB, N_DOM, 768), F32),
            pltpu.VMEM((N_SUB, N_DOM, 768), F32),
            pltpu.VMEM((8, 128), jnp.int32),
            pltpu.SMEM((8, 128), jnp.int32),
            dma,
        ]
        + [dma((N_SUB,))] * 10
        + [dma((N_DOM,))] * 6,
        compiler_params=pltpu.CompilerParams(
            collective_id=0, has_side_effects=True, vmem_limit_bytes=50 * 2**20
        ),
    )(counts, groups, tt, pos, nodes, lists, bins)


def local(
    positions,
    time_bins,
    home_groups,
    targets,
    target_groups,
    node_pos,
    node_mass,
    node_lists,
    list_counts,
):
    tt = jnp.pad(
        jnp.concatenate([targets, target_groups], axis=1).T,
        ((0, 0), (0, 128 - BLK)),
        constant_values=-1,
    )
    nodes = jnp.concatenate([node_pos, node_mass[None]], axis=0)
    pos = jnp.transpose(positions, (1, 0, 2))
    out = whole(list_counts, home_groups, tt, pos, nodes, node_lists, time_bins)
    return jnp.transpose(out, (1, 0, 2))


def solution(mesh):
    return jax.shard_map(
        local,
        mesh=mesh,
        in_specs=(
            P(("dom", "sub"), None, None),
            P(("dom", "sub"), None),
            P(("dom", "sub")),
            P(("dom", "sub"), None),
            P(("dom", "sub"), None),
            P(None, ("dom", "sub")),
            P(("dom", "sub")),
            P("dom", None),
            P("dom"),
        ),
        out_specs=P(("dom", "sub"), None, None),
        check_vma=False,
    )
```

```python
import functools
import jax
import jax.numpy as jnp
from jax import lax
from jax.experimental import pallas as pl
from jax.experimental.pallas import tpu as pltpu
from jax.sharding import PartitionSpec as P

CUR_BIN = 2
LOG2E = 1.4426950408889634
SLOPE = 1.1283791670955126
GROUPS = 64
LIST = 256
N_DOM = 32
N_SUB = 8
TOP = 4
BLK = 64
NODE_DEV = 4096
FIRST = 2
SECOND = 30
SHARE = GROUPS // N_SUB
MESH = pl.DeviceIdType.MESH
F32 = jnp.float32
BF16 = jnp.bfloat16


def thirds(value):
    parts = []
    for _ in range(3):
        part = value.astype(BF16)
        parts.append(part)
        value = value - part.astype(F32)
    return parts


def greet(me_dom, me_sub):
    barrier = pltpu.get_barrier_semaphore()
    for p in range(1, N_SUB):
        pl.semaphore_signal(
            barrier, inc=1, device_id={"sub": lax.rem(me_sub + p, N_SUB)}, device_id_type=MESH
        )

    def one(i, carry):
        pl.semaphore_signal(
            barrier, inc=1, device_id={"dom": lax.rem(me_dom + i, N_DOM)}, device_id_type=MESH
        )
        return carry

    lax.fori_loop(1, N_DOM, one, 0)
    return barrier


def to_sub(src, dst, send, recv, peer, slot, mine):
    return pltpu.make_async_remote_copy(
        src_ref=src,
        dst_ref=dst.at[slot],
        send_sem=send.at[peer],
        recv_sem=recv.at[slot],
        device_id={"sub": peer},
        device_id_type=MESH,
    )


def start_sub(src_of, dst, send, recv, me):
    for p in range(1, N_SUB):
        peer = lax.rem(me + p, N_SUB)
        to_sub(src_of(peer), dst, send, recv, peer, me, me).start()


def wait_sub_recv(src_of, dst, send, recv, me):
    for p in range(1, N_SUB):
        peer = lax.rem(me + p, N_SUB)
        to_sub(src_of(peer), dst, send, recv, peer, peer, me).wait_recv()


def wait_sub_send(src_of, dst, send, recv, me):
    for p in range(1, N_SUB):
        peer = lax.rem(me + p, N_SUB)
        to_sub(src_of(peer), dst, send, recv, peer, me, me).wait_send()


def dom_copy(src, dst, send, recv, peer, slot):
    return pltpu.make_async_remote_copy(
        src_ref=src.at[peer],
        dst_ref=dst.at[slot],
        send_sem=send.at[peer],
        recv_sem=recv.at[slot],
        device_id={"dom": peer},
        device_id_type=MESH,
    )


def each_dom(me, act):
    def one(i, carry):
        act(lax.rem(me + i, N_DOM))
        return carry

    lax.fori_loop(1, N_DOM, one, 0)


def ring_of(me):
    x, core = me // 2, lax.rem(me, 2)
    right = lax.rem(x + 1, N_SUB // 2) * 2 + core
    left = lax.rem(x + 3, N_SUB // 2) * 2 + core
    across = lax.rem(x + 2, N_SUB // 2) * 2 + core
    return me, right, left, across, me + 1 - 2 * core


def other(slot):
    return slot + 1 - 2 * lax.rem(slot, 2)


def ring_copies(own, whole, half, send, recv, ring):
    me, right, left, across, pair = ring

    def one(index, src, dst, sem, dev):
        return pltpu.make_async_remote_copy(
            src_ref=src,
            dst_ref=dst,
            send_sem=send.at[index],
            recv_sem=recv.at[sem],
            device_id={"sub": dev},
            device_id_type=MESH,
        )

    return [
        one(0, own, whole(me), me, right),
        one(1, own, whole(me), me, left),
        one(2, own, whole(me), me, pair),
        one(3, half(left, 0), half(left, 0), N_SUB, right),
        one(4, whole(left), whole(left), left, pair),
        one(5, half(right, 1), half(right, 1), N_SUB + 1, left),
        one(6, whole(right), whole(right), right, pair),
        one(7, whole(across), whole(across), across, pair),
    ]


def ring_wait(whole, half, send, recv, ring, slot, part=None):
    src = whole(slot) if part is None else half(slot, part)
    pltpu.make_async_remote_copy(
        src_ref=src,
        dst_ref=src,
        send_sem=send.at[0],
        recv_sem=recv.at[slot if part is None else N_SUB + part],
        device_id={"sub": ring[4]},
        device_id_type=MESH,
    ).wait_recv()


def ring_one(copies):
    for i in range(3):
        copies[i].start()


def ring_two(copies, wait, ring):
    wait(ring[2])
    copies[3].start()
    copies[4].start()
    wait(ring[1])
    copies[5].start()
    copies[6].start()


def ring_three(copies, wait, ring):
    wait(ring[3], 0)
    wait(ring[3], 1)
    copies[7].start()


def ring_end(wait, ring):
    wait(ring[4])
    for slot in ring[1:4]:
        wait(other(slot))


def build_lists(lists_ref, counts_ref, first_list, tiles, pieces, put):
    highs = tiles.shape[0]
    for c in range(4):
        for p, part in enumerate(thirds(tiles[:, c, :].T)):
            pieces[p, 128 * c : 128 * (c + 1), :] = part

    def one_list(l, carry):
        index = lists_ref[pl.ds(first_list + l, 1), :]
        high = lax.shift_right_logical(index, 7)
        low = jnp.bitwise_and(index, 127)
        pick = lax.broadcasted_iota(jnp.int32, (highs, LIST), 0) == high
        pick = jnp.where(pick, 1.0, 0.0).astype(BF16)
        rows = jnp.zeros((512, LIST), F32)
        for p in range(3):
            rows = rows + jnp.dot(pieces[p], pick, preferred_element_type=F32)
        here = lax.broadcasted_iota(jnp.int32, (128, LIST), 0) == low
        valid = lax.broadcasted_iota(jnp.int32, (1, LIST), 1) < counts_ref[first_list + l]
        picked = [
            jnp.sum(jnp.where(here, rows[128 * c : 128 * (c + 1)], 0.0), axis=0, keepdims=True)
            for c in range(4)
        ]
        mass = jnp.where(valid, -0.25 * picked[3], 0.0)
        put(l, jnp.concatenate([0.5 * picked[0], 0.5 * picked[1], 0.5 * picked[2], mass], axis=0))
        return carry

    lax.fori_loop(0, SHARE, one_list, 0)


def back_copy(src, dst, k, send, recv, peer, slot):
    return pltpu.make_async_remote_copy(
        src_ref=src.at[k, peer],
        dst_ref=dst.at[slot, k],
        send_sem=send.at[peer],
        recv_sem=recv.at[slot],
        device_id={"dom": peer},
        device_id_type=MESH,
    )


def spread_tables(lists, wide):
    pick = lax.broadcasted_iota(jnp.int32, (8, 256), 0)
    side = jnp.where(lax.broadcasted_iota(jnp.int32, (8, 256), 1) < 128, 2, 5)
    pick = jnp.where((pick >= side) & (pick < side + 3), 1.0, 0.0).astype(BF16)

    def one(o, carry):
        for l in range(SHARE):
            t = lists[o, l]
            rows = [t[0:1], t[1:2]]
            for c in (2, 3):
                rows += [part.astype(F32) for part in thirds(t[c : c + 1])]
            t = jnp.concatenate(rows, axis=0).T
            for c in range(2):
                wide[o * SHARE + l, c] = jnp.broadcast_to(t[:, c : c + 1], (LIST, 128))
            both = jnp.dot(t.astype(BF16), pick, preferred_element_type=F32)
            for c in range(2):
                wide[o * SHARE + l, 2 + c] = both[:, 128 * c : 128 * (c + 1)]
        return carry

    lax.fori_loop(0, N_SUB, one, 0)


def visit_sums(wide, row, rows, held):
    sinks = [jnp.broadcast_to(r * 0.5, (8, 128)) for r in rows]
    acc = [jnp.zeros((8, 128), F32) for _ in range(6)]
    for g in range(LIST // 8):
        node = [wide[row, c, 8 * g : 8 * (g + 1), :] for c in range(4)]
        for h in range(2):
            d = [sinks[2 * c + h] - node[c] for c in range(3)]
            s = d[0] * d[0] + (d[1] * d[1] + (d[2] * d[2] + 0.01))
            inv = lax.rsqrt(s)
            e = jnp.exp2(s * (-LOG2E))
            tail = 1.0 - lax.erf(s * inv)
            w = (inv * tail + SLOPE * e) * (inv * inv) * node[3]
            for c in range(3):
                acc[2 * c + h] = acc[2 * c + h] + d[c] * w
    for q in range(6):
        held[q] = acc[q]


def whole_kernel(
    counts_ref,
    groups_ref,
    tt_ref,
    pos_ref,
    nodes_ref,
    lists_ref,
    bins_ref,
    out_ref,
    nrecv,
    tiles,
    pieces,
    crecv,
    precv,
    places,
    chosen,
    codes,
    mid,
    arr,
    trecv,
    hots,
    wide,
    held,
    home,
    pulls,
    ret,
    bsend,
    brecv,
    picked_rows,
    rows_ref,
    rows_sem,
    n_send,
    n_recv,
    c_send,
    c_recv,
    p_send,
    p_recv,
    t_send,
    t_recv,
    b_send,
    b_recv,
    d_send,
    d_recv,
    low_send,
    low_recv,
    high_send,
    high_recv,
):
    me_dom = lax.axis_index("dom")
    me = lax.axis_index("sub")
    barrier = greet(me_dom, me)

    ring = ring_of(me)
    dom_ids = lax.broadcasted_iota(jnp.int32, (N_DOM, 128), 0)
    lanes = lax.broadcasted_iota(jnp.int32, (N_DOM, 128), 1)
    row_ids = lax.broadcasted_iota(jnp.int32, (128, 128), 0)
    col_ids = lax.broadcasted_iota(jnp.int32, (128, 128), 1)

    def pattern(mask):
        return jnp.where(mask, 1.0, 0.0).astype(BF16)

    def count(value, matrix):
        return jnp.dot(value.astype(BF16), matrix, preferred_element_type=F32)

    same = (row_ids < BLK) == (col_ids < BLK)
    earlier = pattern(same & (row_ids < col_ids))
    block = pattern(same)
    crossed = pattern((row_ids < BLK) & (col_ids >= BLK))
    evens, odds = pattern(row_ids < BLK), pattern(row_ids >= BLK)
    full = jnp.ones((128, 128), BF16)
    held[...] = jnp.zeros((6, 8, 128), F32)

    def n_half(slot, h):
        return nrecv.at[slot, :, pl.ds(NODE_DEV // 2 * h, NODE_DEV // 2)]

    def p_half(slot, h):
        return precv.at[slot, :, pl.ds(BLK // 2 * h, BLK // 2)]

    n_whole, p_whole = nrecv.at.__getitem__, precv.at.__getitem__
    n_copies = ring_copies(nodes_ref, n_whole, n_half, n_send, n_recv, ring)
    p_copies = ring_copies(pos_ref, p_whole, p_half, p_send, p_recv, ring)
    n_wait = functools.partial(ring_wait, n_whole, n_half, n_send, n_recv, ring)
    p_wait = functools.partial(ring_wait, p_whole, p_half, p_send, p_recv, ring)

    pl.semaphore_wait(barrier, N_SUB - 1 + N_DOM - 1)
    start_sub(lambda peer: tt_ref, crecv, c_send, c_recv, me)
    ring_one(n_copies)
    ring_one(p_copies)
    crecv[me] = tt_ref[...]
    nrecv[me] = nodes_ref[...]
    precv[me] = pos_ref[...]
    wait_sub_recv(lambda peer: tt_ref, crecv, c_send, c_recv, me)

    base = jnp.zeros((N_DOM, 128), F32)
    marks = [jnp.zeros((N_DOM, 128), F32) for _ in range(2)]
    for pair in range(N_SUB // 2):
        goal = jnp.where(lanes[0:8] < BLK, crecv[2 * pair], crecv[2 * pair + 1])
        wants = [dom_ids == goal[j : j + 1, :] for j in range(TOP)]
        ones_of = [jnp.where(w, 1.0, 0.0) for w in wants]
        stack = jnp.concatenate(ones_of, axis=0)
        within, block_total = count(stack, earlier), count(stack, block)
        summed = (ones_of[0] + ones_of[1]) + (ones_of[2] + ones_of[3])
        start = base + count(summed, crossed)
        base = base + count(summed, full)
        hot = [jnp.zeros((N_DOM, 128), F32) for _ in range(2)]
        for j in range(TOP):
            part = slice(N_DOM * j, N_DOM * (j + 1))
            place = (start + within[part]).astype(jnp.int32)
            start = start + block_total[part]
            places[pair, j] = place
            group = (goal[TOP + j : TOP + j + 1, :] + 1).astype(F32)
            for k in range(2):
                mine = wants[j] & (place == me + N_SUB * k)
                hot[k] = jnp.where(mine, 1.0, hot[k])
                marks[k] = marks[k] + jnp.where(mine, group, 0.0)
        for k in range(2):
            chosen[pair // 2, N_DOM * k : N_DOM * (k + 1), 128 * (pair % 2) : 128 * (pair % 2 + 1)] = (
                hot[k].astype(BF16)
            )
        kinds = hot[0] + 2.0 * hot[1]
        codes[2 * pair] = count(kinds, evens)
        codes[2 * pair + 1] = count(kinds, odds)
    ring_two(n_copies, n_wait, ring)
    own_pair = me // 2
    goal = jnp.where(lanes[0:8] < BLK, crecv[2 * own_pair], crecv[2 * own_pair + 1])
    for t in range(N_SUB):
        hot = jnp.zeros((N_DOM, 128), F32)
        for j in range(TOP):
            mine = (dom_ids == goal[j : j + 1, :]) & (
                jnp.bitwise_and(places[own_pair, j], N_SUB - 1) == t
            )
            hot = jnp.where(mine, 1.0, hot)
        hots[N_DOM * t : N_DOM * (t + 1), :] = hot.astype(BF16)
    for k in range(2):
        mid[:, k, 6, :] = count(marks[k], full)
        mid[:, k, 7, :] = jnp.zeros((N_DOM, 128), F32)
    ring_two(p_copies, p_wait, ring)

    ring_three(n_copies, n_wait, ring)
    ring_end(n_wait, ring)

    def owner_tiles(o, carry):
        for j in range(NODE_DEV // 128):
            tiles[o * (NODE_DEV // 128) + j] = nrecv[o, :, 128 * j : 128 * (j + 1)]
        return carry

    lax.fori_loop(0, N_SUB, owner_tiles, 0)

    def put(l, value):
        trecv[me, l] = value

    build_lists(lists_ref, counts_ref, me * SHARE, tiles, pieces, put)
    start_sub(lambda peer: trecv.at[me], trecv, t_send, t_recv, me)
    ring_three(p_copies, p_wait, ring)
    ring_end(p_wait, ring)

    for c in range(3):
        rows = jnp.zeros((2 * N_DOM, 256), F32)
        for h in range(2):
            some = jnp.concatenate([precv[N_SUB // 2 * h + i, c] for i in range(N_SUB // 2)], axis=0)
            for part in thirds(some):
                rows = rows + jnp.dot(chosen[h], part, preferred_element_type=F32)
        for k in range(2):
            for h in range(2):
                mid[:, k, 2 * c + h, :] = rows[N_DOM * k : N_DOM * (k + 1), 128 * h : 128 * (h + 1)]
    each_dom(me_dom, lambda peer: dom_copy(mid, arr, d_send, d_recv, peer, me_dom).start())
    arr[me_dom] = jnp.zeros((2, 8, 128), F32)
    ret[me_dom] = jnp.zeros((2, 8, 128), F32)

    wait_sub_recv(lambda peer: trecv.at[me], trecv, t_send, t_recv, me)
    spread_tables(trecv, wide)

    def home_rows(v):
        rows = [pos_ref[c, pl.ds(v, 1), :] for c in range(3)]
        return [r[:, 128 * h : 128 * (h + 1)] for r in rows for h in range(2)]

    def home_flush(v):
        for c in range(3):
            parts = [jnp.sum(held[2 * c + h], axis=0, keepdims=True) for h in range(2)]
            home[c, pl.ds(v, 1), :] = jnp.concatenate(parts, axis=1)

    def home_blocks(low, high):
        def one(v, carry):
            home_flush(jnp.maximum(v - 1, low))
            visit_sums(wide, groups_ref[v], home_rows(v), held)
            return carry

        lax.fori_loop(low, high, one, 0)
        home_flush(high - 1)

    home_blocks(0, FIRST)
    each_dom(me_dom, lambda peer: dom_copy(mid, arr, d_send, d_recv, peer, peer).wait_recv())
    diagonal = dom_ids == lax.broadcasted_iota(jnp.int32, (N_DOM, 128), 1)
    marks = [
        jnp.sum(jnp.where(diagonal, arr[:, k, 6, :], 0.0), axis=0, keepdims=True) for k in range(2)
    ]
    marks = jnp.concatenate(marks + [jnp.zeros((6, 128), F32)], axis=0)
    picked_rows[...] = jnp.clip(marks.astype(jnp.int32) - 1, 0, GROUPS - 1)
    to_scalars = pltpu.make_async_copy(picked_rows, rows_ref, rows_sem)
    to_scalars.start()
    to_scalars.wait()

    def imports(k, send, recv):
        def flush(i):
            rows = [jnp.sum(held[q], axis=0, keepdims=True) for q in range(6)]
            rows.append(jnp.zeros((2, 128), F32))
            pulls[k, lax.rem(me_dom + i, N_DOM)] = jnp.concatenate(rows, axis=0)

        def one(i, carry):
            flush(jnp.maximum(i - 1, 1))
            peer = lax.rem(me_dom + i, N_DOM)
            row = rows_ref[k, peer]
            visit_sums(wide, row, [arr[peer, k, q : q + 1, :] for q in range(6)], held)
            return carry

        lax.fori_loop(1, N_DOM, one, 0)
        flush(N_DOM - 1)
        each_dom(me_dom, lambda peer: back_copy(pulls, ret, k, send, recv, peer, me_dom).start())

    imports(0, low_send, low_recv)
    imports(1, high_send, high_recv)

    home_blocks(FIRST, SECOND)

    for k, send, recv in ((0, low_send, low_recv), (1, high_send, high_recv)):
        each_dom(me_dom, lambda peer: back_copy(pulls, ret, k, send, recv, peer, peer).wait_recv())
    for q in range(6):
        low, high = ret[:, 0, q, :], ret[:, 1, q, :]
        for t in range(N_SUB):
            code = codes[t]
            value = jnp.where(code > 1.5, high, jnp.where(code > 0.5, low, 0.0))
            bsend[t, :, 128 * q : 128 * (q + 1)] = value
    start_sub(lambda peer: bsend.at[peer], brecv, b_send, b_recv, me)
    brecv[me] = bsend[me]

    home_blocks(SECOND, BLK)

    wait_sub_recv(lambda peer: bsend.at[peer], brecv, b_send, b_recv, me)
    active = jnp.where(bins_ref[...] <= CUR_BIN, 1.0, 0.0)
    picks = hots[...]
    for c in range(3):
        back = jnp.concatenate([brecv[t, :, 256 * c : 256 * (c + 1)] for t in range(N_SUB)], axis=0)
        total = home[c]
        for part in thirds(back):
            got = lax.dot_general(
                picks, part, (((0,), (0,)), ((), ())), preferred_element_type=F32
            )
            total = total + jnp.where(lax.rem(me, 2) == 0, got[0:BLK], got[BLK : 2 * BLK])
        out_ref[c] = total * active

    wait_sub_send(lambda peer: tt_ref, crecv, c_send, c_recv, me)
    for copy in n_copies + p_copies:
        copy.wait_send()
    wait_sub_send(lambda peer: trecv.at[me], trecv, t_send, t_recv, me)
    wait_sub_send(lambda peer: bsend.at[peer], brecv, b_send, b_recv, me)
    each_dom(me_dom, lambda peer: dom_copy(mid, arr, d_send, d_recv, peer, me_dom).wait_send())
    for k, send, recv in ((0, low_send, low_recv), (1, high_send, high_recv)):
        each_dom(me_dom, lambda peer: back_copy(pulls, ret, k, send, recv, peer, me_dom).wait_send())


def whole(counts, groups, tt, pos, nodes, lists, bins):
    smem = pl.BlockSpec(memory_space=pltpu.SMEM)
    vmem = pl.BlockSpec(memory_space=pltpu.VMEM)
    dma = pltpu.SemaphoreType.DMA
    return pl.pallas_call(
        whole_kernel,
        out_shape=jax.ShapeDtypeStruct((3, BLK, 256), F32),
        in_specs=[smem] * 2 + [vmem] * 5,
        out_specs=vmem,
        scratch_shapes=[
            pltpu.VMEM((N_SUB, 4, NODE_DEV), F32),
            pltpu.VMEM((N_SUB * NODE_DEV // 128, 4, 128), F32),
            pltpu.VMEM((3, 512, N_SUB * NODE_DEV // 128), BF16),
            pltpu.VMEM((N_SUB, 8, 128), jnp.int32),
            pltpu.VMEM((N_SUB, 3, BLK, 256), F32),
            pltpu.VMEM((N_SUB // 2, TOP, N_DOM, 128), jnp.int32),
            pltpu.VMEM((2, 2 * N_DOM, 256), BF16),
            pltpu.VMEM((N_SUB, N_DOM, 128), F32),
            pltpu.VMEM((N_DOM, 2, 8, 128), F32),
            pltpu.VMEM((N_DOM, 2, 8, 128), F32),
            pltpu.VMEM((N_SUB, SHARE, 4, LIST), F32),
            pltpu.VMEM((N_SUB * N_DOM, 128), BF16),
            pltpu.VMEM((GROUPS, 4, LIST, 128), F32),
            pltpu.VMEM((6, 8, 128), F32),
            pltpu.VMEM((3, BLK, 256), F32),
            pltpu.VMEM((2, N_DOM, 8, 128), F32),
            pltpu.VMEM((N_DOM, 2, 8, 128), F32),
            pltpu.VMEM((N_SUB, N_DOM, 768), F32),
            pltpu.VMEM((N_SUB, N_DOM, 768), F32),
            pltpu.VMEM((8, 128), jnp.int32),
            pltpu.SMEM((8, 128), jnp.int32),
            dma,
        ]
        + [dma((N_SUB,)), dma((N_SUB + 2,))]
        + [dma((N_SUB,))] * 2
        + [dma((N_SUB,)), dma((N_SUB + 2,))]
        + [dma((N_SUB,))] * 4
        + [dma((N_DOM,))] * 6,
        compiler_params=pltpu.CompilerParams(
            collective_id=0, has_side_effects=True, vmem_limit_bytes=50 * 2**20
        ),
    )(counts, groups, tt, pos, nodes, lists, bins)


def local(
    positions,
    time_bins,
    home_groups,
    targets,
    target_groups,
    node_pos,
    node_mass,
    node_lists,
    list_counts,
):
    tt = jnp.concatenate([targets, target_groups], axis=1).T
    tt = jnp.concatenate([tt, tt], axis=1)
    nodes = jnp.concatenate([node_pos, node_mass[None]], axis=0)
    pos = jnp.transpose(positions, (1, 0, 2))
    out = whole(list_counts, home_groups, tt, pos, nodes, node_lists, time_bins)
    return jnp.transpose(out, (1, 0, 2))


def solution(mesh):
    return jax.shard_map(
        local,
        mesh=mesh,
        in_specs=(
            P(("dom", "sub"), None, None),
            P(("dom", "sub"), None),
            P(("dom", "sub")),
            P(("dom", "sub"), None),
            P(("dom", "sub"), None),
            P(None, ("dom", "sub")),
            P(("dom", "sub")),
            P("dom", None),
            P("dom"),
        ),
        out_specs=P(("dom", "sub"), None, None),
        check_vma=False,
    )
```

```python
import functools
import jax
import jax.numpy as jnp
from jax import lax
from jax.experimental import pallas as pl
from jax.experimental.pallas import tpu as pltpu
from jax.sharding import PartitionSpec as P

CUR_BIN = 2
LOG2E = 1.4426950408889634
SLOPE = 1.1283791670955126
GROUPS = 64
LIST = 256
N_DOM = 32
N_SUB = 8
TOP = 4
BLK = 64
NODE_DEV = 4096
FIRST = 8
SECOND = 32
SHARE = GROUPS // N_SUB
MESH = pl.DeviceIdType.MESH
F32 = jnp.float32
BF16 = jnp.bfloat16


def thirds(value):
    parts = []
    for _ in range(3):
        part = value.astype(BF16)
        parts.append(part)
        value = value - part.astype(F32)
    return parts


def greet(me_dom, me_sub):
    barrier = pltpu.get_barrier_semaphore()
    for p in range(1, N_SUB):
        pl.semaphore_signal(
            barrier, inc=1, device_id={"sub": lax.rem(me_sub + p, N_SUB)}, device_id_type=MESH
        )

    def one(i, carry):
        pl.semaphore_signal(
            barrier, inc=1, device_id={"dom": lax.rem(me_dom + i, N_DOM)}, device_id_type=MESH
        )
        return carry

    lax.fori_loop(1, N_DOM, one, 0)
    return barrier


def to_sub(src, dst, send, recv, peer, slot, mine):
    return pltpu.make_async_remote_copy(
        src_ref=src,
        dst_ref=dst.at[slot],
        send_sem=send.at[peer],
        recv_sem=recv.at[slot],
        device_id={"sub": peer},
        device_id_type=MESH,
    )


def start_sub(src_of, dst, send, recv, me):
    for p in range(1, N_SUB):
        peer = lax.rem(me + p, N_SUB)
        to_sub(src_of(peer), dst, send, recv, peer, me, me).start()


def wait_sub_recv(src_of, dst, send, recv, me):
    for p in range(1, N_SUB):
        peer = lax.rem(me + p, N_SUB)
        to_sub(src_of(peer), dst, send, recv, peer, peer, me).wait_recv()


def wait_sub_send(src_of, dst, send, recv, me):
    for p in range(1, N_SUB):
        peer = lax.rem(me + p, N_SUB)
        to_sub(src_of(peer), dst, send, recv, peer, me, me).wait_send()


def dom_copy(src, dst, send, recv, me, step):
    return pltpu.make_async_remote_copy(
        src_ref=src.at[step],
        dst_ref=dst.at[N_DOM - step],
        send_sem=send.at[step],
        recv_sem=recv.at[N_DOM - step],
        device_id={"dom": lax.rem(me + step, N_DOM)},
        device_id_type=MESH,
    )


def dom_wait(src, dst, send, recv, me, step):
    pltpu.make_async_remote_copy(
        src_ref=src.at[step],
        dst_ref=dst.at[step],
        send_sem=send.at[step],
        recv_sem=recv.at[step],
        device_id={"dom": lax.rem(me + step, N_DOM)},
        device_id_type=MESH,
    ).wait_recv()


def steps(low, high, act):
    def one(i, carry):
        act(i)
        return carry

    lax.fori_loop(low, high, one, 0)


def ring_of(me):
    x, core = me // 2, lax.rem(me, 2)
    right = lax.rem(x + 1, N_SUB // 2) * 2 + core
    left = lax.rem(x + 3, N_SUB // 2) * 2 + core
    across = lax.rem(x + 2, N_SUB // 2) * 2 + core
    return me, right, left, across, me + 1 - 2 * core


def other(slot):
    return slot + 1 - 2 * lax.rem(slot, 2)


def ring_copies(own, whole, half, send, recv, ring):
    me, right, left, across, pair = ring

    def one(index, src, dst, sem, dev):
        return pltpu.make_async_remote_copy(
            src_ref=src,
            dst_ref=dst,
            send_sem=send.at[index],
            recv_sem=recv.at[sem],
            device_id={"sub": dev},
            device_id_type=MESH,
        )

    return [
        one(0, own, whole(me), me, right),
        one(1, own, whole(me), me, left),
        one(2, own, whole(me), me, pair),
        one(3, half(left, 0), half(left, 0), N_SUB, right),
        one(4, whole(left), whole(left), left, pair),
        one(5, half(right, 1), half(right, 1), N_SUB + 1, left),
        one(6, whole(right), whole(right), right, pair),
        one(7, whole(across), whole(across), across, pair),
    ]


def ring_wait(whole, half, send, recv, ring, slot, part=None):
    src = whole(slot) if part is None else half(slot, part)
    pltpu.make_async_remote_copy(
        src_ref=src,
        dst_ref=src,
        send_sem=send.at[0],
        recv_sem=recv.at[slot if part is None else N_SUB + part],
        device_id={"sub": ring[4]},
        device_id_type=MESH,
    ).wait_recv()


def ring_one(copies):
    for i in range(3):
        copies[i].start()


def ring_two(copies, wait, ring):
    wait(ring[2])
    copies[3].start()
    copies[4].start()
    wait(ring[1])
    copies[5].start()
    copies[6].start()


def ring_three(copies, wait, ring):
    wait(ring[3], 0)
    wait(ring[3], 1)
    copies[7].start()


def ring_end(wait, ring):
    wait(ring[4])
    for slot in ring[1:4]:
        wait(other(slot))


def build_lists(lists_ref, counts_ref, first_list, tiles, pieces, put, midway):
    highs = tiles.shape[0]
    for c in range(4):
        for p, part in enumerate(thirds(tiles[:, c, :].T)):
            pieces[p, 128 * c : 128 * (c + 1), :] = part

    def one_list(l, carry):
        index = lists_ref[pl.ds(first_list + l, 1), :]
        high = lax.shift_right_logical(index, 7)
        low = jnp.bitwise_and(index, 127)
        pick = lax.broadcasted_iota(jnp.int32, (highs, LIST), 0) == high
        pick = jnp.where(pick, 1.0, 0.0).astype(BF16)
        rows = jnp.zeros((512, LIST), F32)
        for p in range(3):
            rows = rows + jnp.dot(pieces[p], pick, preferred_element_type=F32)
        here = lax.broadcasted_iota(jnp.int32, (128, LIST), 0) == low
        valid = lax.broadcasted_iota(jnp.int32, (1, LIST), 1) < counts_ref[first_list + l]
        picked = [
            jnp.sum(jnp.where(here, rows[128 * c : 128 * (c + 1)], 0.0), axis=0, keepdims=True)
            for c in range(4)
        ]
        mass = jnp.where(valid, -0.25 * picked[3], 0.0)
        put(l, jnp.concatenate([0.5 * picked[0], 0.5 * picked[1], 0.5 * picked[2], mass], axis=0))
        return carry

    lax.fori_loop(0, SHARE // 2, one_list, 0)
    midway()
    lax.fori_loop(SHARE // 2, SHARE, one_list, 0)


def spread_tables(lists, wide, low, high, owner):
    pick = lax.broadcasted_iota(jnp.int32, (8, 256), 0)
    side = jnp.where(lax.broadcasted_iota(jnp.int32, (8, 256), 1) < 128, 2, 5)
    pick = jnp.where((pick >= side) & (pick < side + 3), 1.0, 0.0).astype(BF16)

    def one(p, carry):
        o = owner(p)
        for l in range(SHARE):
            t = lists[o, l]
            rows = [t[0:1], t[1:2]]
            for c in (2, 3):
                rows += [part.astype(F32) for part in thirds(t[c : c + 1])]
            t = jnp.concatenate(rows, axis=0).T
            for c in range(2):
                wide[o * SHARE + l, c] = jnp.broadcast_to(t[:, c : c + 1], (LIST, 128))
            both = jnp.dot(t.astype(BF16), pick, preferred_element_type=F32)
            for c in range(2):
                wide[o * SHARE + l, 2 + c] = both[:, 128 * c : 128 * (c + 1)]
        return carry

    lax.fori_loop(low, high, one, 0)


def visit_sums(wide, row, rows, held):
    sinks = [jnp.broadcast_to(r * 0.5, (8, 128)) for r in rows]
    acc = [jnp.zeros((8, 128), F32) for _ in range(6)]
    for g in range(LIST // 8):
        node = [wide[row, c, 8 * g : 8 * (g + 1), :] for c in range(4)]
        for h in range(2):
            d = [sinks[2 * c + h] - node[c] for c in range(3)]
            s = d[0] * d[0] + (d[1] * d[1] + (d[2] * d[2] + 0.01))
            inv = lax.rsqrt(s)
            e = jnp.exp2(s * (-LOG2E))
            tail = 1.0 - lax.erf(s * inv)
            w = (inv * tail + SLOPE * e) * (inv * inv) * node[3]
            for c in range(3):
                acc[2 * c + h] = acc[2 * c + h] + d[c] * w
    for q in range(6):
        held[q] = acc[q]


def whole_kernel(
    counts_ref,
    groups_ref,
    tt_ref,
    pos_ref,
    nodes_ref,
    lists_ref,
    bins_ref,
    out_ref,
    nrecv,
    tiles,
    pieces,
    crecv,
    precv,
    places,
    chosen,
    codes,
    mid,
    arr,
    trecv,
    hots,
    wide,
    held,
    home,
    pulls,
    ret,
    bsend,
    brecv,
    picked_rows,
    rows_ref,
    rows_sem,
    n_send,
    n_recv,
    c_send,
    c_recv,
    p_send,
    p_recv,
    t_send,
    t_recv,
    b_send,
    b_recv,
    e_send,
    e_recv,
    d_send,
    d_recv,
    r_send,
    r_recv,
):
    me_dom = lax.axis_index("dom")
    me = lax.axis_index("sub")
    barrier = greet(me_dom, me)

    ring = ring_of(me)
    dom_ids = lax.broadcasted_iota(jnp.int32, (N_DOM, 128), 0)
    lanes = lax.broadcasted_iota(jnp.int32, (N_DOM, 128), 1)
    row_ids = lax.broadcasted_iota(jnp.int32, (128, 128), 0)
    col_ids = lax.broadcasted_iota(jnp.int32, (128, 128), 1)

    def pattern(mask):
        return jnp.where(mask, 1.0, 0.0).astype(BF16)

    def ahead(goal):
        return jnp.where(goal < 0, -1, jnp.bitwise_and(goal + (N_DOM - me_dom), N_DOM - 1))

    def count(value, matrix):
        return jnp.dot(value.astype(BF16), matrix, preferred_element_type=F32)

    same = (row_ids < BLK) == (col_ids < BLK)
    earlier = pattern(same & (row_ids < col_ids))
    block = pattern(same)
    crossed = pattern((row_ids < BLK) & (col_ids >= BLK))
    evens, odds = pattern(row_ids < BLK), pattern(row_ids >= BLK)
    full = jnp.ones((128, 128), BF16)
    held[...] = jnp.zeros((6, 8, 128), F32)

    def n_half(slot, h):
        return nrecv.at[slot, :, pl.ds(NODE_DEV // 2 * h, NODE_DEV // 2)]

    def p_half(slot, h):
        return precv.at[slot, :, pl.ds(BLK // 2 * h, BLK // 2)]

    n_whole, p_whole = nrecv.at.__getitem__, precv.at.__getitem__
    n_copies = ring_copies(nodes_ref, n_whole, n_half, n_send, n_recv, ring)
    p_copies = ring_copies(pos_ref, p_whole, p_half, p_send, p_recv, ring)
    n_wait = functools.partial(ring_wait, n_whole, n_half, n_send, n_recv, ring)
    p_wait = functools.partial(ring_wait, p_whole, p_half, p_send, p_recv, ring)

    pl.semaphore_wait(barrier, N_SUB - 1 + N_DOM - 1)
    start_sub(lambda peer: tt_ref, crecv, c_send, c_recv, me)
    ring_one(n_copies)
    crecv[me] = tt_ref[...]
    nrecv[me] = nodes_ref[...]
    precv[me] = pos_ref[...]
    wait_sub_recv(lambda peer: tt_ref, crecv, c_send, c_recv, me)

    base = jnp.zeros((N_DOM, 128), F32)
    marks = [jnp.zeros((N_DOM, 128), F32) for _ in range(2)]
    for pair in range(N_SUB // 2):
        goal = jnp.where(lanes[0:8] < BLK, crecv[2 * pair], crecv[2 * pair + 1])
        steps_to = ahead(goal)
        wants = [dom_ids == steps_to[j : j + 1, :] for j in range(TOP)]
        ones_of = [jnp.where(w, 1.0, 0.0) for w in wants]
        stack = jnp.concatenate(ones_of, axis=0)
        within, block_total = count(stack, earlier), count(stack, block)
        summed = (ones_of[0] + ones_of[1]) + (ones_of[2] + ones_of[3])
        start = base + count(summed, crossed)
        base = base + count(summed, full)
        hot = [jnp.zeros((N_DOM, 128), F32) for _ in range(2)]
        for j in range(TOP):
            part = slice(N_DOM * j, N_DOM * (j + 1))
            place = (start + within[part]).astype(jnp.int32)
            start = start + block_total[part]
            places[pair, j] = place
            group = (goal[TOP + j : TOP + j + 1, :] + 1).astype(F32)
            for k in range(2):
                mine = wants[j] & (place == me + N_SUB * k)
                hot[k] = jnp.where(mine, 1.0, hot[k])
                marks[k] = marks[k] + jnp.where(mine, group, 0.0)
        for k in range(2):
            chosen[pair // 2, N_DOM * k : N_DOM * (k + 1), 128 * (pair % 2) : 128 * (pair % 2 + 1)] = (
                hot[k].astype(BF16)
            )
        kinds = hot[0] + 2.0 * hot[1]
        codes[2 * pair] = count(kinds, evens)
        codes[2 * pair + 1] = count(kinds, odds)
    ring_two(n_copies, n_wait, ring)
    ring_one(p_copies)
    own_pair = me // 2
    goal = jnp.where(lanes[0:8] < BLK, crecv[2 * own_pair], crecv[2 * own_pair + 1])
    steps_to = ahead(goal)
    for t in range(N_SUB):
        hot = jnp.zeros((N_DOM, 128), F32)
        for j in range(TOP):
            mine = (dom_ids == steps_to[j : j + 1, :]) & (
                jnp.bitwise_and(places[own_pair, j], N_SUB - 1) == t
            )
            hot = jnp.where(mine, 1.0, hot)
        hots[N_DOM * t : N_DOM * (t + 1), :] = hot.astype(BF16)
    for k in range(2):
        mid[:, k, 6, :] = count(marks[k], full)
        mid[:, k, 7, :] = jnp.zeros((N_DOM, 128), F32)

    ring_three(n_copies, n_wait, ring)
    ring_end(n_wait, ring)

    def owner_tiles(o, carry):
        for j in range(NODE_DEV // 128):
            tiles[o * (NODE_DEV // 128) + j] = nrecv[o, :, 128 * j : 128 * (j + 1)]
        return carry

    lax.fori_loop(0, N_SUB, owner_tiles, 0)

    def put(l, value):
        trecv[me, l] = value

    build_lists(
        lists_ref,
        counts_ref,
        me * SHARE,
        tiles,
        pieces,
        put,
        lambda: ring_two(p_copies, p_wait, ring),
    )
    start_sub(lambda peer: trecv.at[me], trecv, t_send, t_recv, me)
    spread_tables(trecv, wide, 0, 1, lambda p: me + p)
    ring_three(p_copies, p_wait, ring)
    ring_end(p_wait, ring)

    for c in range(3):
        rows = jnp.zeros((2 * N_DOM, 256), F32)
        for h in range(2):
            some = jnp.concatenate([precv[N_SUB // 2 * h + i, c] for i in range(N_SUB // 2)], axis=0)
            for part in thirds(some):
                rows = rows + jnp.dot(chosen[h], part, preferred_element_type=F32)
        for k in range(2):
            for h in range(2):
                mid[:, k, 2 * c + h, :] = rows[N_DOM * k : N_DOM * (k + 1), 128 * h : 128 * (h + 1)]
    steps(1, N_DOM, lambda i: dom_copy(mid, arr, d_send, d_recv, me_dom, i).start())
    arr[0] = jnp.zeros((2, 8, 128), F32)
    ret[0] = jnp.zeros((2, 8, 128), F32)

    def arrived(p):
        peer = lax.rem(me + p, N_SUB)
        to_sub(trecv.at[me], trecv, t_send, t_recv, peer, peer, me).wait_recv()
        return peer

    spread_tables(trecv, wide, 1, N_SUB, arrived)

    def home_rows(v):
        rows = [pos_ref[c, pl.ds(v, 1), :] for c in range(3)]
        return [r[:, 128 * h : 128 * (h + 1)] for r in rows for h in range(2)]

    def home_flush(v):
        for c in range(3):
            parts = [jnp.sum(held[2 * c + h], axis=0, keepdims=True) for h in range(2)]
            home[c, pl.ds(v, 1), :] = jnp.concatenate(parts, axis=1)

    def home_blocks(low, high):
        def one(v, carry):
            home_flush(jnp.maximum(v - 1, low))
            visit_sums(wide, groups_ref[v], home_rows(v), held)
            return carry

        lax.fori_loop(low, high, one, 0)
        home_flush(high - 1)

    home_blocks(0, FIRST)
    steps(1, N_DOM, lambda i: dom_wait(mid, arr, d_send, d_recv, me_dom, i))
    diagonal = dom_ids == lax.broadcasted_iota(jnp.int32, (N_DOM, 128), 1)
    marks = [
        jnp.sum(jnp.where(diagonal, arr[:, k, 6, :], 0.0), axis=0, keepdims=True) for k in range(2)
    ]
    marks = jnp.concatenate(marks + [jnp.zeros((6, 128), F32)], axis=0)
    picked_rows[...] = jnp.clip(marks.astype(jnp.int32) - 1, 0, GROUPS - 1)
    to_scalars = pltpu.make_async_copy(picked_rows, rows_ref, rows_sem)
    to_scalars.start()
    to_scalars.wait()

    def imports(low, high):
        def flush(n):
            rows = [jnp.sum(held[q], axis=0, keepdims=True) for q in range(6)]
            rows.append(jnp.zeros((2, 128), F32))
            pulls[n // 2, lax.rem(n, 2)] = jnp.concatenate(rows, axis=0)

        def one(n, carry):
            flush(jnp.maximum(n - 1, 2 * low))
            i, k = n // 2, lax.rem(n, 2)
            visit_sums(wide, rows_ref[k, i], [arr[i, k, q : q + 1, :] for q in range(6)], held)
            return carry

        lax.fori_loop(2 * low, 2 * high, one, 0)
        flush(2 * high - 1)
        steps(low, high, lambda i: dom_copy(pulls, ret, r_send, r_recv, me_dom, i).start())

    def hand_back(low, send, recv):
        rows = pl.ds(low, N_DOM // 2)
        steps(max(low, 1), low + N_DOM // 2, lambda i: dom_wait(pulls, ret, r_send, r_recv, me_dom, i))
        for q in range(6):
            first, second = ret[rows, 0, q, :], ret[rows, 1, q, :]
            for t in range(N_SUB):
                code = codes[t, rows, :]
                value = jnp.where(code > 1.5, second, jnp.where(code > 0.5, first, 0.0))
                bsend[t, rows, 128 * q : 128 * (q + 1)] = value
        back_part(low, send, recv, True)
        brecv[me, rows] = bsend[me, rows]

    def back_part(low, send, recv, start):
        rows = pl.ds(low, N_DOM // 2)
        for p in range(1, N_SUB):
            peer = lax.rem(me + p, N_SUB)
            copy = pltpu.make_async_remote_copy(
                src_ref=bsend.at[peer, rows],
                dst_ref=brecv.at[me if start else peer, rows],
                send_sem=send.at[peer],
                recv_sem=recv.at[me if start else peer],
                device_id={"sub": peer},
                device_id_type=MESH,
            )
            if start:
                copy.start()
            else:
                copy.wait_recv()
                copy.wait_send()

    half = N_DOM // 2
    imports(half + 1, N_DOM)
    imports(1, half + 1)
    hand_back(0, b_send, b_recv)
    home_blocks(FIRST, SECOND)
    hand_back(half, e_send, e_recv)

    home_blocks(SECOND, BLK)

    back_part(0, b_send, b_recv, False)
    back_part(half, e_send, e_recv, False)
    active = jnp.where(bins_ref[...] <= CUR_BIN, 1.0, 0.0)
    picks = hots[...]
    for c in range(3):
        back = jnp.concatenate([brecv[t, :, 256 * c : 256 * (c + 1)] for t in range(N_SUB)], axis=0)
        total = home[c]
        for part in thirds(back):
            got = lax.dot_general(
                picks, part, (((0,), (0,)), ((), ())), preferred_element_type=F32
            )
            total = total + jnp.where(lax.rem(me, 2) == 0, got[0:BLK], got[BLK : 2 * BLK])
        out_ref[c] = total * active

    wait_sub_send(lambda peer: tt_ref, crecv, c_send, c_recv, me)
    for copy in n_copies + p_copies:
        copy.wait_send()
    wait_sub_send(lambda peer: trecv.at[me], trecv, t_send, t_recv, me)
    steps(1, N_DOM, lambda i: dom_copy(mid, arr, d_send, d_recv, me_dom, i).wait_send())
    steps(1, N_DOM, lambda i: dom_copy(pulls, ret, r_send, r_recv, me_dom, i).wait_send())


def whole(counts, groups, tt, pos, nodes, lists, bins):
    smem = pl.BlockSpec(memory_space=pltpu.SMEM)
    vmem = pl.BlockSpec(memory_space=pltpu.VMEM)
    dma = pltpu.SemaphoreType.DMA
    return pl.pallas_call(
        whole_kernel,
        out_shape=jax.ShapeDtypeStruct((3, BLK, 256), F32),
        in_specs=[smem] * 2 + [vmem] * 5,
        out_specs=vmem,
        scratch_shapes=[
            pltpu.VMEM((N_SUB, 4, NODE_DEV), F32),
            pltpu.VMEM((N_SUB * NODE_DEV // 128, 4, 128), F32),
            pltpu.VMEM((3, 512, N_SUB * NODE_DEV // 128), BF16),
            pltpu.VMEM((N_SUB, 8, 128), jnp.int32),
            pltpu.VMEM((N_SUB, 3, BLK, 256), F32),
            pltpu.VMEM((N_SUB // 2, TOP, N_DOM, 128), jnp.int32),
            pltpu.VMEM((2, 2 * N_DOM, 256), BF16),
            pltpu.VMEM((N_SUB, N_DOM, 128), F32),
            pltpu.VMEM((N_DOM, 2, 8, 128), F32),
            pltpu.VMEM((N_DOM, 2, 8, 128), F32),
            pltpu.VMEM((N_SUB, SHARE, 4, LIST), F32),
            pltpu.VMEM((N_SUB * N_DOM, 128), BF16),
            pltpu.VMEM((GROUPS, 4, LIST, 128), F32),
            pltpu.VMEM((6, 8, 128), F32),
            pltpu.VMEM((3, BLK, 256), F32),
            pltpu.VMEM((N_DOM, 2, 8, 128), F32),
            pltpu.VMEM((N_DOM, 2, 8, 128), F32),
            pltpu.VMEM((N_SUB, N_DOM, 768), F32),
            pltpu.VMEM((N_SUB, N_DOM, 768), F32),
            pltpu.VMEM((8, 128), jnp.int32),
            pltpu.SMEM((8, 128), jnp.int32),
            dma,
        ]
        + [dma((N_SUB,)), dma((N_SUB + 2,))]
        + [dma((N_SUB,))] * 2
        + [dma((N_SUB,)), dma((N_SUB + 2,))]
        + [dma((N_SUB,))] * 6
        + [dma((N_DOM,))] * 4,
        compiler_params=pltpu.CompilerParams(
            collective_id=0, has_side_effects=True, vmem_limit_bytes=50 * 2**20
        ),
    )(counts, groups, tt, pos, nodes, lists, bins)


def local(
    positions,
    time_bins,
    home_groups,
    targets,
    target_groups,
    node_pos,
    node_mass,
    node_lists,
    list_counts,
):
    tt = jnp.concatenate([targets, target_groups], axis=1).T
    tt = jnp.concatenate([tt, tt], axis=1)
    nodes = jnp.concatenate([node_pos, node_mass[None]], axis=0)
    pos = jnp.transpose(positions, (1, 0, 2))
    out = whole(list_counts, home_groups, tt, pos, nodes, node_lists, time_bins)
    return jnp.transpose(out, (1, 0, 2))


def solution(mesh):
    return jax.shard_map(
        local,
        mesh=mesh,
        in_specs=(
            P(("dom", "sub"), None, None),
            P(("dom", "sub"), None),
            P(("dom", "sub")),
            P(("dom", "sub"), None),
            P(("dom", "sub"), None),
            P(None, ("dom", "sub")),
            P(("dom", "sub")),
            P("dom", None),
            P("dom"),
        ),
        out_specs=P(("dom", "sub"), None, None),
        check_vma=False,
    )
```

```python
import functools
import jax
import jax.numpy as jnp
from jax import lax
from jax.experimental import pallas as pl
from jax.experimental.pallas import tpu as pltpu
from jax.sharding import PartitionSpec as P

CUR_BIN = 2
LOG2E = 1.4426950408889634
SLOPE = 1.1283791670955126
GROUPS = 64
LIST = 256
N_DOM = 32
N_SUB = 8
TOP = 4
BLK = 64
NODE_DEV = 4096
FIRST = 14
SECOND = 38
SHARE = GROUPS // N_SUB
MESH = pl.DeviceIdType.MESH
F32 = jnp.float32
BF16 = jnp.bfloat16


def thirds(value):
    parts = []
    for _ in range(3):
        part = value.astype(BF16)
        parts.append(part)
        value = value - part.astype(F32)
    return parts


def greet(me_dom, me_sub):
    barrier = pltpu.get_barrier_semaphore()
    for p in range(1, N_SUB):
        pl.semaphore_signal(
            barrier, inc=1, device_id={"sub": lax.rem(me_sub + p, N_SUB)}, device_id_type=MESH
        )

    def one(i, carry):
        pl.semaphore_signal(
            barrier, inc=1, device_id={"dom": lax.rem(me_dom + i, N_DOM)}, device_id_type=MESH
        )
        return carry

    lax.fori_loop(1, N_DOM, one, 0)
    return barrier


def to_sub(src, dst, send, recv, peer, slot, mine):
    return pltpu.make_async_remote_copy(
        src_ref=src,
        dst_ref=dst.at[slot],
        send_sem=send.at[peer],
        recv_sem=recv.at[slot],
        device_id={"sub": peer},
        device_id_type=MESH,
    )


def start_sub(src_of, dst, send, recv, me):
    for p in range(1, N_SUB):
        peer = lax.rem(me + p, N_SUB)
        to_sub(src_of(peer), dst, send, recv, peer, me, me).start()


def wait_sub_recv(src_of, dst, send, recv, me):
    for p in range(1, N_SUB):
        peer = lax.rem(me + p, N_SUB)
        to_sub(src_of(peer), dst, send, recv, peer, peer, me).wait_recv()


def wait_sub_send(src_of, dst, send, recv, me):
    for p in range(1, N_SUB):
        peer = lax.rem(me + p, N_SUB)
        to_sub(src_of(peer), dst, send, recv, peer, me, me).wait_send()


def dom_copy(src, dst, send, recv, me, step):
    return pltpu.make_async_remote_copy(
        src_ref=src.at[step],
        dst_ref=dst.at[N_DOM - step],
        send_sem=send.at[step],
        recv_sem=recv.at[N_DOM - step],
        device_id={"dom": lax.rem(me + step, N_DOM)},
        device_id_type=MESH,
    )


def dom_wait(src, dst, send, recv, me, step):
    pltpu.make_async_remote_copy(
        src_ref=src.at[step],
        dst_ref=dst.at[step],
        send_sem=send.at[step],
        recv_sem=recv.at[step],
        device_id={"dom": lax.rem(me + step, N_DOM)},
        device_id_type=MESH,
    ).wait_recv()


def steps(low, high, act):
    def one(i, carry):
        act(i)
        return carry

    lax.fori_loop(low, high, one, 0)


def ring_of(me):
    x, core = me // 2, lax.rem(me, 2)
    right = lax.rem(x + 1, N_SUB // 2) * 2 + core
    left = lax.rem(x + 3, N_SUB // 2) * 2 + core
    across = lax.rem(x + 2, N_SUB // 2) * 2 + core
    return me, right, left, across, me + 1 - 2 * core


def other(slot):
    return slot + 1 - 2 * lax.rem(slot, 2)


def ring_copies(own, whole, half, send, recv, ring):
    me, right, left, across, pair = ring

    def one(index, src, dst, sem, dev):
        return pltpu.make_async_remote_copy(
            src_ref=src,
            dst_ref=dst,
            send_sem=send.at[index],
            recv_sem=recv.at[sem],
            device_id={"sub": dev},
            device_id_type=MESH,
        )

    return [
        one(0, own, whole(me), me, right),
        one(1, own, whole(me), me, left),
        one(2, own, whole(me), me, pair),
        one(3, half(left, 0), half(left, 0), N_SUB, right),
        one(4, whole(left), whole(left), left, pair),
        one(5, half(right, 1), half(right, 1), N_SUB + 1, left),
        one(6, whole(right), whole(right), right, pair),
        one(7, whole(across), whole(across), across, pair),
    ]


def ring_wait(whole, half, send, recv, ring, slot, part=None):
    src = whole(slot) if part is None else half(slot, part)
    pltpu.make_async_remote_copy(
        src_ref=src,
        dst_ref=src,
        send_sem=send.at[0],
        recv_sem=recv.at[slot if part is None else N_SUB + part],
        device_id={"sub": ring[4]},
        device_id_type=MESH,
    ).wait_recv()


def ring_one(copies):
    for i in range(3):
        copies[i].start()


def ring_two(copies, wait, ring):
    wait(ring[2])
    copies[3].start()
    copies[4].start()
    wait(ring[1])
    copies[5].start()
    copies[6].start()


def ring_three(copies, wait, ring):
    wait(ring[3], 0)
    wait(ring[3], 1)
    copies[7].start()


def ring_end(wait, ring):
    wait(ring[4])
    for slot in ring[1:4]:
        wait(other(slot))


def build_lists(lists_ref, counts_ref, first_list, tiles, pieces, put, midway):
    highs = tiles.shape[0]
    for c in range(4):
        for p, part in enumerate(thirds(tiles[:, c, :].T)):
            pieces[p, 128 * c : 128 * (c + 1), :] = part

    def one_list(l, carry):
        index = lists_ref[pl.ds(first_list + l, 1), :]
        high = lax.shift_right_logical(index, 7)
        low = jnp.bitwise_and(index, 127)
        pick = lax.broadcasted_iota(jnp.int32, (highs, LIST), 0) == high
        pick = jnp.where(pick, 1.0, 0.0).astype(BF16)
        rows = jnp.zeros((512, LIST), F32)
        for p in range(3):
            rows = rows + jnp.dot(pieces[p], pick, preferred_element_type=F32)
        here = lax.broadcasted_iota(jnp.int32, (128, LIST), 0) == low
        valid = lax.broadcasted_iota(jnp.int32, (1, LIST), 1) < counts_ref[first_list + l]
        picked = [
            jnp.sum(jnp.where(here, rows[128 * c : 128 * (c + 1)], 0.0), axis=0, keepdims=True)
            for c in range(4)
        ]
        mass = jnp.where(valid, -0.25 * picked[3], 0.0)
        put(l, jnp.concatenate([0.5 * picked[0], 0.5 * picked[1], 0.5 * picked[2], mass], axis=0))
        return carry

    lax.fori_loop(0, SHARE // 2, one_list, 0)
    midway()
    lax.fori_loop(SHARE // 2, SHARE, one_list, 0)


def spread_tables(lists, wide, low, high, owner):
    pick = lax.broadcasted_iota(jnp.int32, (8, 256), 0)
    side = jnp.where(lax.broadcasted_iota(jnp.int32, (8, 256), 1) < 128, 2, 5)
    pick = jnp.where((pick >= side) & (pick < side + 3), 1.0, 0.0).astype(BF16)

    def one(p, carry):
        o = owner(p)
        for l in range(SHARE):
            t = lists[o, l]
            rows = [t[0:1], t[1:2]]
            for c in (2, 3):
                rows += [part.astype(F32) for part in thirds(t[c : c + 1])]
            t = jnp.concatenate(rows, axis=0).T
            for c in range(2):
                wide[o * SHARE + l, c] = jnp.broadcast_to(t[:, c : c + 1], (LIST, 128))
            both = jnp.dot(t.astype(BF16), pick, preferred_element_type=F32)
            for c in range(2):
                wide[o * SHARE + l, 2 + c] = both[:, 128 * c : 128 * (c + 1)]
        return carry

    lax.fori_loop(low, high, one, 0)


def visit_sums(wide, row, rows, held):
    sinks = [jnp.broadcast_to(r * 0.5, (8, 128)) for r in rows]
    acc = [jnp.zeros((8, 128), F32) for _ in range(6)]
    for g in range(LIST // 8):
        node = [wide[row, c, 8 * g : 8 * (g + 1), :] for c in range(4)]
        for h in range(2):
            d = [sinks[2 * c + h] - node[c] for c in range(3)]
            s = d[0] * d[0] + (d[1] * d[1] + (d[2] * d[2] + 0.01))
            inv = lax.rsqrt(s)
            e = jnp.exp2(s * (-LOG2E))
            tail = 1.0 - lax.erf(s * inv)
            w = (inv * tail + SLOPE * e) * (inv * inv) * node[3]
            for c in range(3):
                acc[2 * c + h] = acc[2 * c + h] + d[c] * w
    for q in range(6):
        held[q] = acc[q]


def whole_kernel(
    counts_ref,
    groups_ref,
    tt_ref,
    pos_ref,
    nodes_ref,
    lists_ref,
    bins_ref,
    out_ref,
    nrecv,
    tiles,
    pieces,
    crecv,
    precv,
    places,
    chosen,
    codes,
    mid,
    arr,
    trecv,
    hots,
    wide,
    held,
    home,
    pulls,
    ret,
    bsend,
    brecv,
    picked_rows,
    rows_ref,
    rows_sem,
    n_send,
    n_recv,
    c_send,
    c_recv,
    p_send,
    p_recv,
    t_send,
    t_recv,
    b_send,
    b_recv,
    e_send,
    e_recv,
    d_send,
    d_recv,
    r_send,
    r_recv,
):
    me_dom = lax.axis_index("dom")
    me = lax.axis_index("sub")
    barrier = greet(me_dom, me)

    ring = ring_of(me)
    dom_ids = lax.broadcasted_iota(jnp.int32, (N_DOM, 128), 0)
    lanes = lax.broadcasted_iota(jnp.int32, (N_DOM, 128), 1)
    row_ids = lax.broadcasted_iota(jnp.int32, (128, 128), 0)
    col_ids = lax.broadcasted_iota(jnp.int32, (128, 128), 1)

    def pattern(mask):
        return jnp.where(mask, 1.0, 0.0).astype(BF16)

    def ahead(goal):
        return jnp.where(goal < 0, -1, jnp.bitwise_and(goal + (N_DOM - me_dom), N_DOM - 1))

    def count(value, matrix):
        return jnp.dot(value.astype(BF16), matrix, preferred_element_type=F32)

    same = (row_ids < BLK) == (col_ids < BLK)
    earlier = pattern(same & (row_ids < col_ids))
    block = pattern(same)
    crossed = pattern((row_ids < BLK) & (col_ids >= BLK))
    evens, odds = pattern(row_ids < BLK), pattern(row_ids >= BLK)
    full = jnp.ones((128, 128), BF16)
    held[...] = jnp.zeros((6, 8, 128), F32)

    def n_half(slot, h):
        return nrecv.at[slot, :, pl.ds(NODE_DEV // 2 * h, NODE_DEV // 2)]

    def p_half(slot, h):
        return precv.at[slot, :, pl.ds(BLK // 2 * h, BLK // 2)]

    n_whole, p_whole = nrecv.at.__getitem__, precv.at.__getitem__
    n_copies = ring_copies(nodes_ref, n_whole, n_half, n_send, n_recv, ring)
    p_copies = ring_copies(pos_ref, p_whole, p_half, p_send, p_recv, ring)
    n_wait = functools.partial(ring_wait, n_whole, n_half, n_send, n_recv, ring)
    p_wait = functools.partial(ring_wait, p_whole, p_half, p_send, p_recv, ring)

    pl.semaphore_wait(barrier, N_SUB - 1 + N_DOM - 1)
    start_sub(lambda peer: tt_ref, crecv, c_send, c_recv, me)
    ring_one(n_copies)
    crecv[me] = tt_ref[...]
    nrecv[me] = nodes_ref[...]
    precv[me] = pos_ref[...]
    wait_sub_recv(lambda peer: tt_ref, crecv, c_send, c_recv, me)

    base = jnp.zeros((N_DOM, 128), F32)
    marks = [jnp.zeros((N_DOM, 128), F32) for _ in range(2)]
    for pair in range(N_SUB // 2):
        goal = jnp.where(lanes[0:8] < BLK, crecv[2 * pair], crecv[2 * pair + 1])
        steps_to = ahead(goal)
        wants = [dom_ids == steps_to[j : j + 1, :] for j in range(TOP)]
        ones_of = [jnp.where(w, 1.0, 0.0) for w in wants]
        stack = jnp.concatenate(ones_of, axis=0)
        within, block_total = count(stack, earlier), count(stack, block)
        summed = (ones_of[0] + ones_of[1]) + (ones_of[2] + ones_of[3])
        start = base + count(summed, crossed)
        base = base + count(summed, full)
        hot = [jnp.zeros((N_DOM, 128), F32) for _ in range(2)]
        for j in range(TOP):
            part = slice(N_DOM * j, N_DOM * (j + 1))
            place = (start + within[part]).astype(jnp.int32)
            start = start + block_total[part]
            places[pair, j] = place
            group = (goal[TOP + j : TOP + j + 1, :] + 1).astype(F32)
            for k in range(2):
                mine = wants[j] & (place == me + N_SUB * k)
                hot[k] = jnp.where(mine, 1.0, hot[k])
                marks[k] = marks[k] + jnp.where(mine, group, 0.0)
        for k in range(2):
            chosen[pair // 2, N_DOM * k : N_DOM * (k + 1), 128 * (pair % 2) : 128 * (pair % 2 + 1)] = (
                hot[k].astype(BF16)
            )
        kinds = hot[0] + 2.0 * hot[1]
        codes[2 * pair] = count(kinds, evens)
        codes[2 * pair + 1] = count(kinds, odds)
    ring_two(n_copies, n_wait, ring)
    ring_one(p_copies)
    own_pair = me // 2
    goal = jnp.where(lanes[0:8] < BLK, crecv[2 * own_pair], crecv[2 * own_pair + 1])
    steps_to = ahead(goal)
    for t in range(N_SUB):
        hot = jnp.zeros((N_DOM, 128), F32)
        for j in range(TOP):
            mine = (dom_ids == steps_to[j : j + 1, :]) & (
                jnp.bitwise_and(places[own_pair, j], N_SUB - 1) == t
            )
            hot = jnp.where(mine, 1.0, hot)
        hots[N_DOM * t : N_DOM * (t + 1), :] = hot.astype(BF16)
    for k in range(2):
        mid[:, k, 6, :] = count(marks[k], full)
        mid[:, k, 7, :] = jnp.zeros((N_DOM, 128), F32)

    ring_three(n_copies, n_wait, ring)
    ring_end(n_wait, ring)

    def owner_tiles(o, carry):
        for j in range(NODE_DEV // 128):
            tiles[o * (NODE_DEV // 128) + j] = nrecv[o, :, 128 * j : 128 * (j + 1)]
        return carry

    lax.fori_loop(0, N_SUB, owner_tiles, 0)

    def put(l, value):
        trecv[me, l] = value

    build_lists(
        lists_ref,
        counts_ref,
        me * SHARE,
        tiles,
        pieces,
        put,
        lambda: ring_two(p_copies, p_wait, ring),
    )
    start_sub(lambda peer: trecv.at[me], trecv, t_send, t_recv, me)
    spread_tables(trecv, wide, 0, 1, lambda p: me + p)
    ring_three(p_copies, p_wait, ring)
    ring_end(p_wait, ring)

    for c in range(3):
        rows = jnp.zeros((2 * N_DOM, 256), F32)
        for h in range(2):
            some = jnp.concatenate([precv[N_SUB // 2 * h + i, c] for i in range(N_SUB // 2)], axis=0)
            for part in thirds(some):
                rows = rows + jnp.dot(chosen[h], part, preferred_element_type=F32)
        for k in range(2):
            for h in range(2):
                mid[:, k, 2 * c + h, :] = rows[N_DOM * k : N_DOM * (k + 1), 128 * h : 128 * (h + 1)]
    steps(1, N_DOM, lambda i: dom_copy(mid, arr, d_send, d_recv, me_dom, i).start())
    arr[0] = jnp.zeros((2, 8, 128), F32)
    ret[0] = jnp.zeros((2, 8, 128), F32)

    def arrived(p):
        peer = lax.rem(me + p, N_SUB)
        to_sub(trecv.at[me], trecv, t_send, t_recv, peer, peer, me).wait_recv()
        return peer

    spread_tables(trecv, wide, 1, N_SUB, arrived)

    def home_rows(v):
        rows = [pos_ref[c, pl.ds(v, 1), :] for c in range(3)]
        return [r[:, 128 * h : 128 * (h + 1)] for r in rows for h in range(2)]

    def home_flush(v):
        for c in range(3):
            parts = [jnp.sum(held[2 * c + h], axis=0, keepdims=True) for h in range(2)]
            home[c, pl.ds(v, 1), :] = jnp.concatenate(parts, axis=1)

    def home_blocks(low, high):
        def one(v, carry):
            home_flush(jnp.maximum(v - 1, low))
            visit_sums(wide, groups_ref[v], home_rows(v), held)
            return carry

        lax.fori_loop(low, high, one, 0)
        home_flush(high - 1)

    home_blocks(0, FIRST)
    steps(1, N_DOM, lambda i: dom_wait(mid, arr, d_send, d_recv, me_dom, i))
    diagonal = dom_ids == lax.broadcasted_iota(jnp.int32, (N_DOM, 128), 1)
    marks = [
        jnp.sum(jnp.where(diagonal, arr[:, k, 6, :], 0.0), axis=0, keepdims=True) for k in range(2)
    ]
    marks = jnp.concatenate(marks + [jnp.zeros((6, 128), F32)], axis=0)
    picked_rows[...] = jnp.clip(marks.astype(jnp.int32) - 1, 0, GROUPS - 1)
    to_scalars = pltpu.make_async_copy(picked_rows, rows_ref, rows_sem)
    to_scalars.start()
    to_scalars.wait()

    def imports(low, high):
        def flush(n):
            rows = [jnp.sum(held[q], axis=0, keepdims=True) for q in range(6)]
            rows.append(jnp.zeros((2, 128), F32))
            pulls[n // 2, lax.rem(n, 2)] = jnp.concatenate(rows, axis=0)

        def one(n, carry):
            flush(jnp.maximum(n - 1, 2 * low))
            i, k = n // 2, lax.rem(n, 2)
            visit_sums(wide, rows_ref[k, i], [arr[i, k, q : q + 1, :] for q in range(6)], held)
            return carry

        lax.fori_loop(2 * low, 2 * high, one, 0)
        flush(2 * high - 1)
        steps(low, high, lambda i: dom_copy(pulls, ret, r_send, r_recv, me_dom, i).start())

    def hand_back(low, send, recv):
        rows = pl.ds(low, N_DOM // 2)
        steps(max(low, 1), low + N_DOM // 2, lambda i: dom_wait(pulls, ret, r_send, r_recv, me_dom, i))
        for q in range(6):
            first, second = ret[rows, 0, q, :], ret[rows, 1, q, :]
            for t in range(N_SUB):
                code = codes[t, rows, :]
                value = jnp.where(code > 1.5, second, jnp.where(code > 0.5, first, 0.0))
                bsend[t, rows, 128 * q : 128 * (q + 1)] = value
        back_part(low, send, recv, True)
        brecv[me, rows] = bsend[me, rows]

    def back_part(low, send, recv, start):
        rows = pl.ds(low, N_DOM // 2)
        for p in range(1, N_SUB):
            peer = lax.rem(me + p, N_SUB)
            copy = pltpu.make_async_remote_copy(
                src_ref=bsend.at[peer, rows],
                dst_ref=brecv.at[me if start else peer, rows],
                send_sem=send.at[peer],
                recv_sem=recv.at[me if start else peer],
                device_id={"sub": peer},
                device_id_type=MESH,
            )
            if start:
                copy.start()
            else:
                copy.wait_recv()
                copy.wait_send()

    half = N_DOM // 2
    imports(half + 1, N_DOM)
    imports(1, half + 1)
    hand_back(0, b_send, b_recv)
    home_blocks(FIRST, SECOND)
    hand_back(half, e_send, e_recv)

    home_blocks(SECOND, BLK)

    back_part(0, b_send, b_recv, False)
    back_part(half, e_send, e_recv, False)
    active = jnp.where(bins_ref[...] <= CUR_BIN, 1.0, 0.0)
    picks = hots[...]
    for c in range(3):
        back = jnp.concatenate([brecv[t, :, 256 * c : 256 * (c + 1)] for t in range(N_SUB)], axis=0)
        total = home[c]
        for part in thirds(back):
            got = lax.dot_general(
                picks, part, (((0,), (0,)), ((), ())), preferred_element_type=F32
            )
            total = total + jnp.where(lax.rem(me, 2) == 0, got[0:BLK], got[BLK : 2 * BLK])
        out_ref[c] = total * active

    wait_sub_send(lambda peer: tt_ref, crecv, c_send, c_recv, me)
    for copy in n_copies + p_copies:
        copy.wait_send()
    wait_sub_send(lambda peer: trecv.at[me], trecv, t_send, t_recv, me)
    steps(1, N_DOM, lambda i: dom_copy(mid, arr, d_send, d_recv, me_dom, i).wait_send())
    steps(1, N_DOM, lambda i: dom_copy(pulls, ret, r_send, r_recv, me_dom, i).wait_send())


def whole(counts, groups, tt, pos, nodes, lists, bins):
    smem = pl.BlockSpec(memory_space=pltpu.SMEM)
    vmem = pl.BlockSpec(memory_space=pltpu.VMEM)
    dma = pltpu.SemaphoreType.DMA
    return pl.pallas_call(
        whole_kernel,
        out_shape=jax.ShapeDtypeStruct((3, BLK, 256), F32),
        in_specs=[smem] * 2 + [vmem] * 5,
        out_specs=vmem,
        scratch_shapes=[
            pltpu.VMEM((N_SUB, 4, NODE_DEV), F32),
            pltpu.VMEM((N_SUB * NODE_DEV // 128, 4, 128), F32),
            pltpu.VMEM((3, 512, N_SUB * NODE_DEV // 128), BF16),
            pltpu.VMEM((N_SUB, 8, 128), jnp.int32),
            pltpu.VMEM((N_SUB, 3, BLK, 256), F32),
            pltpu.VMEM((N_SUB // 2, TOP, N_DOM, 128), jnp.int32),
            pltpu.VMEM((2, 2 * N_DOM, 256), BF16),
            pltpu.VMEM((N_SUB, N_DOM, 128), F32),
            pltpu.VMEM((N_DOM, 2, 8, 128), F32),
            pltpu.VMEM((N_DOM, 2, 8, 128), F32),
            pltpu.VMEM((N_SUB, SHARE, 4, LIST), F32),
            pltpu.VMEM((N_SUB * N_DOM, 128), BF16),
            pltpu.VMEM((GROUPS, 4, LIST, 128), F32),
            pltpu.VMEM((6, 8, 128), F32),
            pltpu.VMEM((3, BLK, 256), F32),
            pltpu.VMEM((N_DOM, 2, 8, 128), F32),
            pltpu.VMEM((N_DOM, 2, 8, 128), F32),
            pltpu.VMEM((N_SUB, N_DOM, 768), F32),
            pltpu.VMEM((N_SUB, N_DOM, 768), F32),
            pltpu.VMEM((8, 128), jnp.int32),
            pltpu.SMEM((8, 128), jnp.int32),
            dma,
        ]
        + [dma((N_SUB,)), dma((N_SUB + 2,))]
        + [dma((N_SUB,))] * 2
        + [dma((N_SUB,)), dma((N_SUB + 2,))]
        + [dma((N_SUB,))] * 6
        + [dma((N_DOM,))] * 4,
        compiler_params=pltpu.CompilerParams(
            collective_id=0, has_side_effects=True, vmem_limit_bytes=50 * 2**20
        ),
    )(counts, groups, tt, pos, nodes, lists, bins)


def local(
    positions,
    time_bins,
    home_groups,
    targets,
    target_groups,
    node_pos,
    node_mass,
    node_lists,
    list_counts,
):
    tt = jnp.concatenate([targets, target_groups], axis=1).T
    tt = jnp.concatenate([tt, tt], axis=1)
    nodes = jnp.concatenate([node_pos, node_mass[None]], axis=0)
    pos = jnp.transpose(positions, (1, 0, 2))
    out = whole(list_counts, home_groups, tt, pos, nodes, node_lists, time_bins)
    return jnp.transpose(out, (1, 0, 2))


def solution(mesh):
    return jax.shard_map(
        local,
        mesh=mesh,
        in_specs=(
            P(("dom", "sub"), None, None),
            P(("dom", "sub"), None),
            P(("dom", "sub")),
            P(("dom", "sub"), None),
            P(("dom", "sub"), None),
            P(None, ("dom", "sub")),
            P(("dom", "sub")),
            P("dom", None),
            P("dom"),
        ),
        out_specs=P(("dom", "sub"), None, None),
        check_vma=False,
    )
```
